32 devices in a mesh: gy: 16 (over z, x, core), gz: 2 (over y).
Axes of the slice: x: 2, y: 2, z: 4, core: 2. Of those that a mesh axis runs over, the one named last changes fastest.
Arguments:
- populations: float32 [19, 4, 128, 2048], P(None, None, 'gy', 'gz'), may hold values from 0 to 1, as said below
- solid_mask: int32 [4, 128, 2048], P(None, 'gy', 'gz'), may hold values 0 or 1
- body_force: float32 [3], replicated, may hold values from 0.002 to 0.008
Outputs:
- density: float32 [4, 128, 2048], P(None, 'gy', 'gz')
- velocity: float32 [3, 4, 128, 2048], P(None, None, 'gy', 'gz')
The draws below stay inside these ranges and needn't reach their ends.
Inputs may be any that keep to these rules, and one draw needn't show every extreme that they name: `populations`: every population is positive, near its lattice weight times one.
All inputs are finite; a program needn't handle non-finite values. No bound on the sum of `solid_mask` on one device may be relied on, other than what follows from the above.
Results may differ from the reference program's by a relative error of at most 0.0003.
Values sent between devices are 32-bit elements; how exact they have to be, the bound alone decides.
A program may use at most 64 MiB of HBM per device.

```python
import jax
import jax.numpy as jnp
from jax import lax

PLANES = 4
STEPS = 3
NY = 128
NZ = 2048


def draw_populations(key, part):
    weight_list = [1.0 / 3.0] + [1.0 / 18.0] * 6 + [1.0 / 36.0] * 12
    lift_list = [0, 0, 0, 0, 0, 1, -1, 0, 0, 0, 0, 1, -1, -1, 1, 1, -1, -1, 1]
    wfull = jnp.asarray(weight_list, dtype=jnp.float32).reshape(19, 1, 1, 1)
    lift = jnp.asarray(lift_list, dtype=jnp.float32).reshape(19, 1, 1, 1)
    shape = (19, PLANES, NY, NZ)
    rough = 1.0 + jax.random.uniform(key, shape, jnp.float32, -0.4, 0.4)
    return wfull * rough * (1.0 + 0.09 * lift)


def with_ends(values, key, least, top_value):
    longest = values.shape.index(max(values.shape))
    spots = []
    for shift in (0, 1):
        where = [jax.random.randint(jax.random.fold_in(key, axis), (), 0, length) for axis, length in enumerate(values.shape)]
        where[longest] = (where[longest] + shift) % values.shape[longest]
        spots.append(tuple(where))
    return values.at[spots[0]].set(least).at[spots[1]].set(top_value)


def setup_inputs(seed: int = 0) -> dict:
    streams_of = jax.random.split(jax.random.key(seed), 4)
    return {
        "populations": draw_populations(jax.random.fold_in(streams_of[3], 71), 0),
        "solid_mask": with_ends((jax.random.randint(streams_of[1], (PLANES, NY, NZ), 0, 4) < 1).astype(jnp.int32), jax.random.fold_in(streams_of[1], 1), 0, 1),
        "body_force": jnp.clip(jax.random.uniform(streams_of[2], (3,), jnp.float32, 0.002, 0.008), 0.002, 0.008),
    }


velocities = [(0, 0, 0), (1, 0, 0), (-1, 0, 0), (0, 1, 0), (0, -1, 0), (0, 0, 1), (0, 0, -1),
              (1, 1, 0), (-1, -1, 0), (1, -1, 0), (-1, 1, 0), (1, 0, 1), (-1, 0, -1),
              (1, 0, -1), (-1, 0, 1), (0, 1, 1), (0, -1, -1), (0, 1, -1), (0, -1, 1)]
opposite = [0, 2, 1, 4, 3, 6, 5, 8, 7, 10, 9, 12, 11, 14, 13, 16, 15, 18, 17]
lattice_weights = [1.0 / 3.0] + [1.0 / 18.0] * 6 + [1.0 / 36.0] * 12
reference_mach = 0.05


def invert_list(matrix):
    count = len(matrix)
    work = [list(matrix[i]) + [1.0 if i == j else 0.0 for j in range(count)] for i in range(count)]
    for column in range(count):
        pivot = column
        for row in range(column + 1, count):
            if abs(work[row][column]) > abs(work[pivot][column]):
                pivot = row
        work[column], work[pivot] = work[pivot], work[column]
        factor = work[column][column]
        work[column] = [entry / factor for entry in work[column]]
        for row in range(count):
            if row != column:
                scale = work[row][column]
                if scale != 0.0:
                    work[row] = [a - scale * b for a, b in zip(work[row], work[column])]
    return [line[count:] for line in work]


def relax_table():
    columns = []
    for shift_x, shift_y, shift_z in velocities:
        columns.append([1, shift_x, shift_y, shift_z, shift_x ** 2, shift_y ** 2, shift_z ** 2,
                        shift_x * shift_y, shift_x * shift_z, shift_y * shift_z,
                        shift_x ** 2 * shift_y, shift_x ** 2 * shift_z, shift_y ** 2 * shift_x,
                        shift_y ** 2 * shift_z, shift_z ** 2 * shift_x, shift_z ** 2 * shift_y,
                        shift_x ** 2 * shift_y ** 2, shift_x ** 2 * shift_z ** 2, shift_y ** 2 * shift_z ** 2])
    moments = [[float(columns[k][a]) for k in range(19)] for a in range(19)]
    inverse = invert_list(moments)
    rates = [0.0] * 4 + [1.25] * 6 + [1.6] * 6 + [1.3] * 3
    table = [[sum(inverse[i][a] * rates[a] * moments[a][j] for a in range(19)) for j in range(19)]
             for i in range(19)]
    return jnp.asarray(table, dtype=jnp.float32)


def collide(current, body_force, relax):
    cvec = jnp.asarray(velocities, dtype=jnp.float32)
    wvec = jnp.asarray(lattice_weights, dtype=jnp.float32)
    wfull = wvec.reshape(19, 1, 1, 1)
    density = jnp.sum(current, axis=0)
    momentum = jnp.tensordot(cvec.T, current, axes=1, precision=lax.Precision.HIGHEST)
    flow = momentum / density
    projected = jnp.tensordot(cvec, flow, axes=1, precision=lax.Precision.HIGHEST)
    speed_sq = jnp.sum(flow * flow, axis=0)
    equilibrium = wfull * density * (1.0 + 3.0 * projected + 4.5 * projected * projected - 1.5 * speed_sq)
    departure = (current - equilibrium).reshape(19, -1)
    change = jnp.dot(relax, departure, precision=lax.Precision.HIGHEST).reshape(current.shape)
    forcing = 3.0 * wvec * jnp.dot(cvec, body_force, precision=lax.Precision.HIGHEST)
    return current - change + forcing.reshape(19, 1, 1, 1)


def stream(padded, solid_pad, center):
    planes, across, length = center.shape[1:]
    result = []
    for k in range(19):
        shift_x, shift_y, shift_z = velocities[k]
        source = padded[k, 1 - shift_x:1 - shift_x + planes, 1 - shift_y:1 - shift_y + across,
                        1 - shift_z:1 - shift_z + length]
        blocked = solid_pad[1 - shift_x:1 - shift_x + planes, 1 - shift_y:1 - shift_y + across,
                            1 - shift_z:1 - shift_z + length]
        result.append(jnp.where(blocked > 0, center[opposite[k]], source))
    return jnp.stack(result)


def moments_out(current, solid_core):
    cvec = jnp.asarray(velocities, dtype=jnp.float32)
    fluid = (1 - solid_core).astype(jnp.float32)
    density = jnp.sum(current, axis=0)
    momentum = jnp.tensordot(cvec.T, current, axes=1, precision=lax.Precision.HIGHEST)
    return density * fluid, momentum / density / reference_mach * fluid


def reference(populations, solid_mask, body_force):
    relax = relax_table()
    solid_pad = jnp.pad(solid_mask, ((0, 0), (1, 1), (1, 1)), mode="wrap")
    solid_pad = jnp.pad(solid_pad, ((1, 1), (0, 0), (0, 0)), constant_values=1)
    current = populations
    for sweep in range(STEPS):
        relaxed = collide(current, body_force, relax)
        padded = jnp.pad(relaxed, ((0, 0), (0, 0), (1, 1), (1, 1)), mode="wrap")
        padded = jnp.pad(padded, ((0, 0), (1, 1), (0, 0), (0, 0)))
        current = stream(padded, solid_pad, relaxed)
    return moments_out(current, solid_mask)
```

```python
import functools

import jax
import jax.numpy as jnp
from jax import lax
from jax.experimental import pallas as pl
from jax.experimental.pallas import tpu as pltpu
from jax.sharding import PartitionSpec as P

STEPS = 3
W = 128
SEG = 8
VMEM_LIMIT = 60 << 20
LO, HI, ROWS = 8, 16, 24

velocities = [
    (0, 0, 0),
    (1, 0, 0),
    (-1, 0, 0),
    (0, 1, 0),
    (0, -1, 0),
    (0, 0, 1),
    (0, 0, -1),
    (1, 1, 0),
    (-1, -1, 0),
    (1, -1, 0),
    (-1, 1, 0),
    (1, 0, 1),
    (-1, 0, -1),
    (1, 0, -1),
    (-1, 0, 1),
    (0, 1, 1),
    (0, -1, -1),
    (0, 1, -1),
    (0, -1, 1),
]
opposite = [0, 2, 1, 4, 3, 6, 5, 8, 7, 10, 9, 12, 11, 14, 13, 16, 15, 18, 17]
reference_mach = 0.05
ORDER = [5, 11, 14, 15, 3, 7, 10, 17, 6, 12, 13, 16, 4, 8, 9, 18, 0, 1, 2]
SLOT = [ORDER.index(k) for k in range(19)]
Y_RUN = {1: [(3, 5)], -1: [(11, 5)]}
Z_RUN = {1: [(0, 4), (15, 1)], -1: [(7, 5)]}
SIDES = [(1, 0), (-1, 0), (0, 1), (0, -1), (1, 1), (-1, 1), (1, -1), (-1, -1)]
MESH = pl.DeviceIdType.MESH


def moments(f):
    s = [f[2 * a + 1] + f[2 * a + 2] for a in range(9)]
    d = [f[2 * a + 1] - f[2 * a + 2] for a in range(9)]
    axes = s[0] + s[1] + s[2]
    a = (s[3] + s[4], s[5] + s[6], s[7] + s[8])
    edges = a[0] + a[1] + a[2]
    rho = f[0] + axes + edges
    px, py, pz = (d[3] + d[4]) + (d[5] + d[6]), (d[3] - d[4]) + (d[7] + d[8]), (d[5] - d[6]) + (d[7] - d[8])
    jx, jy, jz = d[0] + px, d[1] + py, d[2] + pz
    return s, d, a, (axes, edges), (px, py, pz), rho, jx, jy, jz


def collide(f, force):
    s, d, (axy, axz, ayz), (axes, edges), p, rho, jx, jy, jz = moments(f)
    w = 0.3125 / rho
    vx, vy, vz = jx * w, jy * w, jz * w
    rx, ry, rz = jx * vx, jy * vy, jz * vz
    r = rx + ry + rz
    r3 = r * (0.325 / 0.9375)
    common = rho * (0.625 / 3.0 - 1.3 / 9.0) - r3
    fourth = rho * (0.325 / 9.0) + r3
    out = [None] * 19
    out[0] = (rho * (1.3 / 3.0 - 0.25) - r * 1.92) + (axes * 0.25 + edges * 0.2)
    g = [j * (0.4 / 3.0) + force[i][0] for i, j in enumerate((jx, jy, jz))]
    along = (axy + axz, axy + ayz, axz + ayz)
    for i, ri in enumerate((rx, ry, rz)):
        even = (common + ri * 0.96) + (along[i] * 0.025 - s[i] * 0.125)
        odd = (p[i] * 0.3 - g[i] * 0.25) + force[i][1]
        out[2 * i + 1] = even + odd
        out[2 * i + 2] = even - odd
    planes = (
        (3, axy, rz, vx * jy, g[0], g[1]),
        (5, axz, ry, vx * jz, g[0], g[2]),
        (7, ayz, rx, vy * jz, g[1], g[2]),
    )
    for n, total, across, shear, ga, gb in planes:
        a = (fourth - across * 0.52) - total * 0.075
        b = shear - (s[n] - s[n + 1]) * 0.0625
        e0, e1 = a + b, a - b
        o0, o1 = (ga + gb) - d[n] * 0.3, (ga - gb) - d[n + 1] * 0.3
        out[2 * n + 1], out[2 * n + 2] = e0 + o0, e0 - o0
        out[2 * n + 3], out[2 * n + 4] = e1 + o1, e1 - o1
    return out


def kernel(gy, gz, pop_hbm, mask_hbm, force_hbm, out_ref, raw, raw_mask, force_ref, cells0, cells1, cells2, mask,
           moved_mask, load_sem, send_sem, recv_sem):
    state = (cells0, cells1, cells2)
    planes, across = mask.shape[1], mask.shape[0] - 2
    my, mz = lax.axis_index("gy"), lax.axis_index("gz")

    def peer(dy, dz):
        return {"gy": lax.rem(my + dy + gy, gy), "gz": lax.rem(mz + dz + gz, gz)}

    load_mask = pltpu.make_async_copy(mask_hbm, raw_mask, load_sem.at[0])
    load_force = pltpu.make_async_copy(force_hbm, force_ref, load_sem.at[1])
    load_pop = [pltpu.make_async_copy(pop_hbm.at[:, p], raw.at[:, p], load_sem.at[2 + p]) for p in range(planes)]
    load_mask.start()
    load_force.start()
    for copy in load_pop:
        copy.start()
    barrier = pltpu.get_barrier_semaphore()
    for dy, dz in SIDES:
        pl.semaphore_signal(barrier, inc=1, device_id=peer(dy, dz), device_id_type=MESH)

    lane = lax.broadcasted_iota(jnp.int32, (SEG, W), 1)
    line = slice(LO, HI)

    def remote(source, target, number, side):
        return pltpu.make_async_remote_copy(
            src_ref=source,
            dst_ref=target,
            send_sem=send_sem.at[number],
            recv_sem=recv_sem.at[number],
            device_id=peer(*side),
            device_id_type=MESH,
        )

    def edge(dy):
        return (across, 0) if dy == 1 else (1, across + 1)

    def ends(dz):
        return (slice(HI - 1, HI), slice(LO - 1, LO)) if dz == 1 else (slice(LO, LO + 1), slice(HI, HI + 1))

    count = [0]

    def next_sem():
        count[0] += 1
        return count[0] - 1

    def start(group):
        for copy in group:
            copy.start()
        return group

    def arrive(group):
        for copy in group:
            copy.wait_recv()

    sent = []

    def send_y(buf, dy):
        here, there = edge(dy)
        group = [
            remote(state[buf].at[pl.ds(a, n), here, :, line], state[buf].at[pl.ds(a, n), there, :, line], next_sem(), (dy, 0))
            for a, n in Y_RUN[dy]
        ]
        for dz in (1, -1):
            src, dst = ends(dz)
            k = SLOT[velocities.index((0, dy, dz))]
            group.append(remote(state[buf].at[k, here, :, src], state[buf].at[k, there, :, dst], next_sem(), (dy, dz)))
        sent.append(start(group))
        return group

    def send_z(buf, rows):
        group = []
        for dz in (1, -1):
            src, dst = ends(dz)
            for a, n in Z_RUN[dz]:
                for y0, ny in rows:
                    group.append(
                        remote(
                            state[buf].at[pl.ds(a, n), pl.ds(y0, ny), :, src],
                            state[buf].at[pl.ds(a, n), pl.ds(y0, ny), :, dst],
                            next_sem(),
                            (0, dz),
                        )
                    )
        sent.append(start(group))
        return group

    def send_mask():
        group = []
        for dy in (1, -1):
            here, there = edge(dy)
            group.append(remote(mask.at[here, :, line], mask.at[there, :, line], next_sem(), (dy, 0)))
        for dz in (1, -1):
            src, dst = ends(dz)
            group.append(remote(mask.at[pl.ds(1, across), :, src], mask.at[pl.ds(1, across), :, dst], next_sem(), (0, dz)))
            for dy in (1, -1):
                here, there = edge(dy)
                group.append(remote(mask.at[here, :, src], mask.at[there, :, dst], next_sem(), (dy, dz)))
        sent.append(start(group))
        return group

    def along_z(load, cz):
        v = load(0)
        if cz == 1:
            return pltpu.roll(jnp.where(lane == W - 1, load(-1), v), 1, 1)
        if cz == -1:
            return pltpu.roll(jnp.where(lane == 0, load(1), v), W - 1, 1)
        return v

    def move_mask(y):
        for p in range(planes):
            for i, cz in enumerate((1, -1)):
                moved_mask[i, y, p] = along_z(lambda o: mask[y, p, LO + o : HI + o, :], cz)

    def streamed(buf, p, y):
        f = []
        for k in range(19):
            cx, cy, cz = velocities[k]
            here = state[buf][SLOT[opposite[k]], y, p, line, :]
            q = p - cx
            if k == 0 or not 0 <= q < planes:
                f.append(here)
                continue
            moved = along_z(lambda o: state[buf][SLOT[k], y - cy, q, LO + o : HI + o, :], cz)
            blocked = mask[y - cy, q, line, :] if cz == 0 else moved_mask[(1 - cz) // 2, y - cy, q]
            f.append(jnp.where(blocked != 0, here, moved))
        return f

    def relax(buf, f, p, y):
        for k, value in enumerate(collide(f, force)):
            state[buf][SLOT[k], y, p, line, :] = value

    load_mask.wait()
    for p in range(planes):
        for y in range(across):
            mask[y + 1, p, line, :] = raw_mask[p, pl.ds(y, SEG, stride=across), :]
    load_force.wait()
    force = [(force_ref[i] * (1.0 / 12.0), force_ref[i] * 0.1875) for i in range(3)]

    group = max(u for u in (4, 2, 1) if across % u == 0)
    for p in range(planes):
        load_pop[p].wait()

        def first(i, carry, p=p):
            for n in range(group):
                y = i * group + n
                relax(0, [raw[k, p, pl.ds(y, SEG, stride=across), :] for k in range(19)], p, y + 1)
            return carry

        lax.fori_loop(0, across // group, first, 0)

    pl.semaphore_wait(barrier, len(SIDES))
    coming_mask = send_mask()
    coming_y = {dy: send_y(0, dy) for dy in (1, -1)}
    coming_z = send_z(0, [(1, across)])

    arrive(coming_mask)

    def shift(y, carry):
        move_mask(y)
        return carry

    lax.fori_loop(0, across + 2, shift, 0)

    def final(buf, y):
        for p in range(planes):
            rho, jx, jy, jz = moments(streamed(buf, p, y))[-4:]
            fluid = (1 - mask[y, p, line, :]).astype(jnp.float32)
            scale = fluid * (1.0 / reference_mach) / rho
            spot = pl.ds(y - 1, SEG, stride=across)
            out_ref[0, p, spot, :] = rho * fluid
            out_ref[1, p, spot, :] = jx * scale
            out_ref[2, p, spot, :] = jy * scale
            out_ref[3, p, spot, :] = jz * scale

    def middle(step, y):
        for p in range(planes):
            relax(step + 1, streamed(step, p, y), p, y)

    def interior(block):
        def body(y, carry):
            block(y)
            return carry

        lax.fori_loop(3, across - 1, body, 0)

    near, far = coming_z, coming_z
    for step in range(STEPS - 1):
        arrive(near)
        later_y = {}
        for dy, y in ((-1, 1), (1, across)):
            arrive(coming_y[-dy])
            middle(step, y)
            later_y[dy] = send_y(step + 1, dy)
        if far is not near:
            arrive(far)
        middle(step, 2)
        middle(step, across - 1)
        near = send_z(step + 1, [(1, 2), (across - 1, 2)])
        interior(functools.partial(middle, step))
        far = send_z(step + 1, [(3, across - 4)])
        coming_y = later_y

    last = STEPS - 1
    arrive(near)
    arrive(far)
    final(last, 2)
    final(last, across - 1)
    interior(functools.partial(final, last))
    for dy, y in ((-1, 1), (1, across)):
        arrive(coming_y[-dy])
        final(last, y)
    for group in sent:
        for copy in group:
            copy.wait_send()


def hand_out(both_ref, den_hbm, vel_hbm, sem):
    den = pltpu.make_async_copy(both_ref.at[0], den_hbm, sem.at[0])
    vel = pltpu.make_async_copy(both_ref.at[pl.ds(1, 3)], vel_hbm, sem.at[1])
    vel.start()
    den.start()
    vel.wait()
    den.wait()


def solution(mesh):
    gy, gz = mesh.shape["gy"], mesh.shape["gz"]

    def tiles(x, across):
        lead = x.shape[:-2]
        x = x.reshape(*lead, across, SEG, W)
        return jnp.swapaxes(x, -3, -2).reshape(*lead, SEG * across, W)

    def lines(x, across):
        lead = x.shape[:-2]
        x = x.reshape(*lead, SEG, across, W)
        return jnp.swapaxes(x, -3, -2).reshape(*lead, across, SEG * W)

    def local(populations, solid_mask, body_force):
        planes, across, length = solid_mask.shape
        if length != SEG * W or across < 6:
            raise ValueError("unsupported block")
        messages = 64
        both = pl.pallas_call(
            functools.partial(kernel, gy, gz),
            out_shape=jax.ShapeDtypeStruct((4, planes, SEG * across, W), jnp.float32),
            in_specs=[pl.BlockSpec(memory_space=pltpu.HBM)] * 3,
            out_specs=pl.BlockSpec(memory_space=pltpu.VMEM),
            scratch_shapes=[
                pltpu.VMEM((19, planes, SEG * across, W), jnp.float32),
                pltpu.VMEM((planes, SEG * across, W), jnp.int32),
                pltpu.SMEM((3,), jnp.float32),
                *[pltpu.VMEM((19, across + 2, planes, ROWS, W), jnp.float32)] * STEPS,
                pltpu.VMEM((across + 2, planes, ROWS, W), jnp.int32),
                pltpu.VMEM((2, across + 2, planes, SEG, W), jnp.int32),
                pltpu.SemaphoreType.DMA((2 + planes,)),
                pltpu.SemaphoreType.DMA((messages,)),
                pltpu.SemaphoreType.DMA((messages,)),
            ],
            compiler_params=pltpu.CompilerParams(collective_id=0, has_side_effects=True, vmem_limit_bytes=VMEM_LIMIT),
        )(tiles(populations, across), tiles(solid_mask, across), body_force)
        density, velocity = pl.pallas_call(
            hand_out,
            out_shape=(
                jax.ShapeDtypeStruct((planes, SEG * across, W), jnp.float32),
                jax.ShapeDtypeStruct((3, planes, SEG * across, W), jnp.float32),
            ),
            in_specs=[pl.BlockSpec(memory_space=pltpu.VMEM)],
            out_specs=(pl.BlockSpec(memory_space=pl.ANY), pl.BlockSpec(memory_space=pl.ANY)),
            scratch_shapes=[pltpu.SemaphoreType.DMA((2,))],
            compiler_params=pltpu.CompilerParams(vmem_limit_bytes=VMEM_LIMIT),
        )(both)
        return lines(density, across), lines(velocity, across)

    return jax.shard_map(
        local,
        mesh=mesh,
        in_specs=(P(None, None, "gy", "gz"), P(None, "gy", "gz"), P()),
        out_specs=(P(None, "gy", "gz"), P(None, None, "gy", "gz")),
        check_vma=False,
    )
```

```python
import functools

import jax
import jax.numpy as jnp
from jax import lax
from jax.experimental import pallas as pl
from jax.experimental.pallas import tpu as pltpu
from jax.sharding import PartitionSpec as P

STEPS = 3
W = 128
SEG = 8
VMEM_LIMIT = 60 << 20
LO, HI, ROWS = 8, 16, 24

velocities = [
    (0, 0, 0),
    (1, 0, 0),
    (-1, 0, 0),
    (0, 1, 0),
    (0, -1, 0),
    (0, 0, 1),
    (0, 0, -1),
    (1, 1, 0),
    (-1, -1, 0),
    (1, -1, 0),
    (-1, 1, 0),
    (1, 0, 1),
    (-1, 0, -1),
    (1, 0, -1),
    (-1, 0, 1),
    (0, 1, 1),
    (0, -1, -1),
    (0, 1, -1),
    (0, -1, 1),
]
opposite = [0, 2, 1, 4, 3, 6, 5, 8, 7, 10, 9, 12, 11, 14, 13, 16, 15, 18, 17]
reference_mach = 0.05
ORDER = [5, 11, 14, 15, 3, 7, 10, 17, 6, 12, 13, 16, 4, 8, 9, 18, 0, 1, 2]
SLOT = [ORDER.index(k) for k in range(19)]
Y_RUN = {1: [(3, 5)], -1: [(11, 5)]}
Z_SET = {dz: [k for k in range(19) if velocities[k][2] == dz] for dz in (1, -1)}
SIDES = [(1, 0), (-1, 0), (0, 1), (0, -1), (1, 1), (-1, 1), (1, -1), (-1, -1)]
MESH = pl.DeviceIdType.MESH


def moments(f):
    s = [f[2 * a + 1] + f[2 * a + 2] for a in range(9)]
    d = [f[2 * a + 1] - f[2 * a + 2] for a in range(9)]
    axes = s[0] + s[1] + s[2]
    a = (s[3] + s[4], s[5] + s[6], s[7] + s[8])
    edges = a[0] + a[1] + a[2]
    rho = f[0] + axes + edges
    px, py, pz = (d[3] + d[4]) + (d[5] + d[6]), (d[3] - d[4]) + (d[7] + d[8]), (d[5] - d[6]) + (d[7] - d[8])
    jx, jy, jz = d[0] + px, d[1] + py, d[2] + pz
    return s, d, a, (axes, edges), (px, py, pz), rho, jx, jy, jz


def collide(f, force):
    s, d, (axy, axz, ayz), (axes, edges), p, rho, jx, jy, jz = moments(f)
    w = 0.3125 / rho
    vx, vy, vz = jx * w, jy * w, jz * w
    rx, ry, rz = jx * vx, jy * vy, jz * vz
    r = rx + ry + rz
    r3 = r * (0.325 / 0.9375)
    common = rho * (0.625 / 3.0 - 1.3 / 9.0) - r3
    fourth = rho * (0.325 / 9.0) + r3
    out = [None] * 19
    out[0] = (rho * (1.3 / 3.0 - 0.25) - r * 1.92) + (axes * 0.25 + edges * 0.2)
    g = [j * (0.4 / 3.0) + force[i][0] for i, j in enumerate((jx, jy, jz))]
    along = (axy + axz, axy + ayz, axz + ayz)
    for i, ri in enumerate((rx, ry, rz)):
        even = (common + ri * 0.96) + (along[i] * 0.025 - s[i] * 0.125)
        odd = (p[i] * 0.3 - g[i] * 0.25) + force[i][1]
        out[2 * i + 1] = even + odd
        out[2 * i + 2] = even - odd
    planes = (
        (3, axy, rz, vx * jy, g[0], g[1]),
        (5, axz, ry, vx * jz, g[0], g[2]),
        (7, ayz, rx, vy * jz, g[1], g[2]),
    )
    for n, total, across, shear, ga, gb in planes:
        a = (fourth - across * 0.52) - total * 0.075
        b = shear - (s[n] - s[n + 1]) * 0.0625
        e0, e1 = a + b, a - b
        o0, o1 = (ga + gb) - d[n] * 0.3, (ga - gb) - d[n + 1] * 0.3
        out[2 * n + 1], out[2 * n + 2] = e0 + o0, e0 - o0
        out[2 * n + 3], out[2 * n + 4] = e1 + o1, e1 - o1
    return out


def kernel(gy, gz, pop_hbm, mask_hbm, force_hbm, out_ref, raw, raw_mask, force_ref, cells0, cells1, cells2, mask,
           moved_mask, zs, zh, mzs, mzh, load_sem, send_sem, recv_sem):
    state = (cells0, cells1, cells2)
    planes, across = pop_hbm.shape[1], pop_hbm.shape[2] // SEG
    my, mz = lax.axis_index("gy"), lax.axis_index("gz")

    def peer(dy, dz):
        return {"gy": lax.rem(my + dy + gy, gy), "gz": lax.rem(mz + dz + gz, gz)}

    load_mask = pltpu.make_async_copy(mask_hbm, raw_mask, load_sem.at[0])
    load_force = pltpu.make_async_copy(force_hbm, force_ref, load_sem.at[1])
    load_pop = [pltpu.make_async_copy(pop_hbm.at[:, p], raw.at[:, p], load_sem.at[2 + p]) for p in range(planes)]
    load_mask.start()
    load_force.start()
    for copy in load_pop:
        copy.start()
    barrier = pltpu.get_barrier_semaphore()
    for dy, dz in SIDES:
        pl.semaphore_signal(barrier, inc=1, device_id=peer(dy, dz), device_id_type=MESH)

    lane = lax.broadcasted_iota(jnp.int32, (SEG, W), 1)
    line = slice(LO, HI)

    def remote(source, target, number, side):
        return pltpu.make_async_remote_copy(
            src_ref=source,
            dst_ref=target,
            send_sem=send_sem.at[number],
            recv_sem=recv_sem.at[number],
            device_id=peer(*side),
            device_id_type=MESH,
        )

    def edge(dy):
        return (across, 0) if dy == 1 else (1, across + 1)

    def ends(dz):
        return (slice(HI - 1, HI), slice(LO - 1, LO)) if dz == 1 else (slice(LO, LO + 1), slice(HI, HI + 1))

    count = [0]

    def next_sem():
        count[0] += 1
        return count[0] - 1

    def start(group):
        for copy in group:
            copy.start()
        return group

    def arrive(group):
        for copy in group:
            copy.wait_recv()

    sent = []

    def entries(ref, lead):
        return ref.reshape(*lead, across + 2, planes, ROWS, W)

    views = [entries(ref, (19,)) for ref in state]
    mask_view = entries(mask, ())

    def at(y, p, row=LO):
        base = (y * planes + p) * ROWS
        return (base if isinstance(y, int) else pl.multiple_of(base, 8)) + row

    def send_y(buf, dy):
        here, there = edge(dy)
        group = []
        for dz in (1, -1):
            src, dst = ends(dz)
            k = SLOT[velocities.index((0, dy, dz))]
            group.append(remote(views[buf].at[k, here, :, src], views[buf].at[k, there, :, dst], next_sem(), (dy, dz)))
        for a, n in Y_RUN[dy]:
            source, target = views[buf].at[pl.ds(a, n), here, :, line], views[buf].at[pl.ds(a, n), there, :, line]
            group.append(remote(source, target, next_sem(), (dy, 0)))
        sent.append(start(group))
        return group

    def send_z(out, into, lines_of, starts, group):
        copies = []
        for i, dz in enumerate((1, -1)):
            refs = lines_of(dz)
            packed = jnp.zeros((SEG, W), out.dtype)
            row = HI - 1 if dz == 1 else LO
            for j, (load, y) in enumerate((load, y) for load, _ in refs for y in starts):
                shift = (j + 1 if dz == 1 else j) % W
                v = load(pl.ds(at(y, 0, row), SEG, stride=ROWS))
                packed = jnp.where(lane == j, pltpu.roll(v, shift, 1) if shift else v, packed)
            out[group, i] = packed
            copies.append(remote(out.at[group, i], into.at[group, i], next_sem(), (0, dz)))
        sent.append(start(copies))

        def done():
            for i, dz in enumerate((1, -1)):
                copies[i].wait_recv()
                row = LO - 1 if dz == 1 else HI
                packed = into[group, i]
                for j, (store, y) in enumerate((store, y) for _, store in lines_of(dz) for y in starts):
                    shift = (W - 1 - j if dz == 1 else W - j) % W
                    store(pl.ds(at(y, 0, row), SEG, stride=ROWS), pltpu.roll(packed, shift, 1) if shift else packed)

        return done

    def lines_of(ref):
        def pick(dz):
            result = []
            for k in Z_SET[dz]:
                slot = SLOT[k]

                def load(rows, slot=slot):
                    return ref[slot, rows, :]

                def store(rows, value, slot=slot):
                    ref[slot, rows, :] = value

                result.append((load, store))
            return result

        return pick

    def mask_lines(dz):
        def store(rows, value):
            mask[rows, :] = value

        return [(lambda rows: mask[rows, :], store)]

    near_rows, far_rows = [1, across - 1], list(range(3, across - 1, 2))

    def send_state(buf, rows):
        group = buf * 2 + (0 if rows is near_rows else 1)
        return send_z(zs, zh, lines_of(state[buf]), rows, group)

    def send_mask():
        group = []
        for dy in (1, -1):
            here, there = edge(dy)
            for dz in (1, -1):
                src, dst = ends(dz)
                group.append(remote(mask_view.at[here, :, src], mask_view.at[there, :, dst], next_sem(), (dy, dz)))
            group.append(remote(mask_view.at[here, :, line], mask_view.at[there, :, line], next_sem(), (dy, 0)))
        sent.append(start(group))
        return group, send_z(mzs, mzh, mask_lines, near_rows + far_rows, 0)

    def along_z(load, cz):
        v = load(0)
        if cz == 1:
            return pltpu.roll(jnp.where(lane == W - 1, load(-1), v), 1, 1)
        if cz == -1:
            return pltpu.roll(jnp.where(lane == 0, load(1), v), W - 1, 1)
        return v

    def move_mask(y):
        for p in range(planes):
            for i, cz in enumerate((1, -1)):
                moved_mask[i, y, p] = along_z(lambda o: mask[pl.ds(at(y, p, LO + o), SEG), :], cz)

    def streamed(buf, p, y):
        f = []
        for k in range(19):
            cx, cy, cz = velocities[k]
            here = state[buf][SLOT[opposite[k]], pl.ds(at(y, p), SEG), :]
            q = p - cx
            if k == 0 or not 0 <= q < planes:
                f.append(here)
                continue
            moved = along_z(lambda o: state[buf][SLOT[k], pl.ds(at(y - cy, q, LO + o), SEG), :], cz)
            blocked = mask[pl.ds(at(y - cy, q), SEG), :] if cz == 0 else moved_mask[(1 - cz) // 2, y - cy, q]
            f.append(jnp.where(blocked != 0, here, moved))
        return f

    def relax(buf, f, p, y):
        for k, value in enumerate(collide(f, force)):
            state[buf][SLOT[k], pl.ds(at(y, p), SEG), :] = value

    load_mask.wait()
    for p in range(planes):
        for y in range(across):
            mask[pl.ds(at(y + 1, p), SEG), :] = raw_mask[p, pl.ds(y, SEG, stride=across), :]
    load_force.wait()
    force = [(force_ref[i] * (1.0 / 12.0), force_ref[i] * 0.1875) for i in range(3)]

    group = max(u for u in (4, 2, 1) if across % u == 0)
    for p in range(planes):
        load_pop[p].wait()

        def first(i, carry, p=p):
            for n in range(group):
                y = i * group + n
                relax(0, [raw[k, p, pl.ds(y, SEG, stride=across), :] for k in range(19)], p, y + 1)
            return carry

        lax.fori_loop(0, across // group, first, 0)

    pl.semaphore_wait(barrier, len(SIDES))
    coming_mask, mask_done = send_mask()
    coming_y = {dy: send_y(0, dy) for dy in (1, -1)}
    near, far = send_state(0, near_rows), send_state(0, far_rows)

    mask_done()
    arrive(coming_mask)

    def shift(y, carry):
        move_mask(y)
        return carry

    lax.fori_loop(0, across + 2, shift, 0)

    def final(buf, y):
        for p in range(planes):
            rho, jx, jy, jz = moments(streamed(buf, p, y))[-4:]
            fluid = (1 - mask[pl.ds(at(y, p), SEG), :]).astype(jnp.float32)
            scale = fluid * (1.0 / reference_mach) / rho
            spot = pl.ds(y - 1, SEG, stride=across)
            out_ref[0, p, spot, :] = rho * fluid
            out_ref[1, p, spot, :] = jx * scale
            out_ref[2, p, spot, :] = jy * scale
            out_ref[3, p, spot, :] = jz * scale

    def middle(step, y):
        for p in range(planes):
            relax(step + 1, streamed(step, p, y), p, y)

    def interior(block):
        def body(y, carry):
            block(y)
            return carry

        lax.fori_loop(3, across - 1, body, 0)

    for step in range(STEPS - 1):
        near()
        later_y = {}
        for dy, y in ((-1, 1), (1, across)):
            arrive(coming_y[-dy])
            middle(step, y)
            later_y[dy] = send_y(step + 1, dy)
        far()
        middle(step, 2)
        middle(step, across - 1)
        near = send_state(step + 1, near_rows)
        interior(functools.partial(middle, step))
        far = send_state(step + 1, far_rows)
        coming_y = later_y

    last = STEPS - 1
    near()
    far()
    final(last, 2)
    final(last, across - 1)
    interior(functools.partial(final, last))
    for dy, y in ((-1, 1), (1, across)):
        arrive(coming_y[-dy])
        final(last, y)
    for group in sent:
        for copy in group:
            copy.wait_send()


def hand_out(both_ref, den_hbm, vel_hbm, sem):
    den = pltpu.make_async_copy(both_ref.at[0], den_hbm, sem.at[0])
    vel = pltpu.make_async_copy(both_ref.at[pl.ds(1, 3)], vel_hbm, sem.at[1])
    vel.start()
    den.start()
    vel.wait()
    den.wait()


def solution(mesh):
    gy, gz = mesh.shape["gy"], mesh.shape["gz"]

    def tiles(x, across):
        lead = x.shape[:-2]
        x = x.reshape(*lead, across, SEG, W)
        return jnp.swapaxes(x, -3, -2).reshape(*lead, SEG * across, W)

    def lines(x, across):
        lead = x.shape[:-2]
        x = x.reshape(*lead, SEG, across, W)
        return jnp.swapaxes(x, -3, -2).reshape(*lead, across, SEG * W)

    def local(populations, solid_mask, body_force):
        planes, across, length = solid_mask.shape
        if length != SEG * W or across < 6 or across % 2 or 2 * planes != SEG:
            raise ValueError("unsupported block")
        messages = 64
        both = pl.pallas_call(
            functools.partial(kernel, gy, gz),
            out_shape=jax.ShapeDtypeStruct((4, planes, SEG * across, W), jnp.float32),
            in_specs=[pl.BlockSpec(memory_space=pltpu.HBM)] * 3,
            out_specs=pl.BlockSpec(memory_space=pltpu.VMEM),
            scratch_shapes=[
                pltpu.VMEM((19, planes, SEG * across, W), jnp.float32),
                pltpu.VMEM((planes, SEG * across, W), jnp.int32),
                pltpu.SMEM((3,), jnp.float32),
                *[pltpu.VMEM((19, (across + 2) * planes * ROWS, W), jnp.float32)] * STEPS,
                pltpu.VMEM(((across + 2) * planes * ROWS, W), jnp.int32),
                pltpu.VMEM((2, across + 2, planes, SEG, W), jnp.int32),
                pltpu.VMEM((2 * STEPS, 2, SEG, W), jnp.float32),
                pltpu.VMEM((2 * STEPS, 2, SEG, W), jnp.float32),
                pltpu.VMEM((1, 2, SEG, W), jnp.int32),
                pltpu.VMEM((1, 2, SEG, W), jnp.int32),
                pltpu.SemaphoreType.DMA((2 + planes,)),
                pltpu.SemaphoreType.DMA((messages,)),
                pltpu.SemaphoreType.DMA((messages,)),
            ],
            compiler_params=pltpu.CompilerParams(collective_id=0, has_side_effects=True, vmem_limit_bytes=VMEM_LIMIT),
        )(tiles(populations, across), tiles(solid_mask, across), body_force)
        density, velocity = pl.pallas_call(
            hand_out,
            out_shape=(
                jax.ShapeDtypeStruct((planes, SEG * across, W), jnp.float32),
                jax.ShapeDtypeStruct((3, planes, SEG * across, W), jnp.float32),
            ),
            in_specs=[pl.BlockSpec(memory_space=pltpu.VMEM)],
            out_specs=(pl.BlockSpec(memory_space=pl.ANY), pl.BlockSpec(memory_space=pl.ANY)),
            scratch_shapes=[pltpu.SemaphoreType.DMA((2,))],
            compiler_params=pltpu.CompilerParams(vmem_limit_bytes=1 << 20),
        )(both)
        return lines(density, across), lines(velocity, across)

    return jax.shard_map(
        local,
        mesh=mesh,
        in_specs=(P(None, None, "gy", "gz"), P(None, "gy", "gz"), P()),
        out_specs=(P(None, "gy", "gz"), P(None, None, "gy", "gz")),
        check_vma=False,
    )
```

```python
import functools

import jax
import jax.numpy as jnp
from jax import lax
from jax.experimental import pallas as pl
from jax.experimental.pallas import tpu as pltpu
from jax.sharding import PartitionSpec as P

STEPS = 3
W = 128
SEG = 8
VMEM_LIMIT = 60 << 20
LO, HI, ROWS = 8, 16, 24

velocities = [
    (0, 0, 0),
    (1, 0, 0),
    (-1, 0, 0),
    (0, 1, 0),
    (0, -1, 0),
    (0, 0, 1),
    (0, 0, -1),
    (1, 1, 0),
    (-1, -1, 0),
    (1, -1, 0),
    (-1, 1, 0),
    (1, 0, 1),
    (-1, 0, -1),
    (1, 0, -1),
    (-1, 0, 1),
    (0, 1, 1),
    (0, -1, -1),
    (0, 1, -1),
    (0, -1, 1),
]
opposite = [0, 2, 1, 4, 3, 6, 5, 8, 7, 10, 9, 12, 11, 14, 13, 16, 15, 18, 17]
reference_mach = 0.05
ORDER = [5, 11, 14, 15, 3, 7, 10, 17, 6, 12, 13, 16, 4, 8, 9, 18, 0, 1, 2]
SLOT = [ORDER.index(k) for k in range(19)]
Y_RUN = {1: [(3, 5)], -1: [(11, 5)]}
Z_SET = {dz: [k for k in range(19) if velocities[k][2] == dz] for dz in (1, -1)}
SIDES = [(1, 0), (-1, 0), (0, 1), (0, -1), (1, 1), (-1, 1), (1, -1), (-1, -1)]
MESH = pl.DeviceIdType.MESH


def moments(f):
    s = [f[2 * a + 1] + f[2 * a + 2] for a in range(9)]
    d = [f[2 * a + 1] - f[2 * a + 2] for a in range(9)]
    axes = s[0] + s[1] + s[2]
    a = (s[3] + s[4], s[5] + s[6], s[7] + s[8])
    edges = a[0] + a[1] + a[2]
    rho = f[0] + axes + edges
    px, py, pz = (d[3] + d[4]) + (d[5] + d[6]), (d[3] - d[4]) + (d[7] + d[8]), (d[5] - d[6]) + (d[7] - d[8])
    jx, jy, jz = d[0] + px, d[1] + py, d[2] + pz
    return s, d, a, (axes, edges), (px, py, pz), rho, jx, jy, jz


def collide(f, force):
    s, d, (axy, axz, ayz), (axes, edges), p, rho, jx, jy, jz = moments(f)
    w = 0.3125 / rho
    vx, vy, vz = jx * w, jy * w, jz * w
    rx, ry, rz = jx * vx, jy * vy, jz * vz
    r = rx + ry + rz
    r3 = r * (0.325 / 0.9375)
    common = rho * (0.625 / 3.0 - 1.3 / 9.0) - r3
    fourth = rho * (0.325 / 9.0) + r3
    out = [None] * 19
    out[0] = (rho * (1.3 / 3.0 - 0.25) - r * 1.92) + (axes * 0.25 + edges * 0.2)
    g = [j * (0.4 / 3.0) + force[i][0] for i, j in enumerate((jx, jy, jz))]
    along = (axy + axz, axy + ayz, axz + ayz)
    for i, ri in enumerate((rx, ry, rz)):
        even = (common + ri * 0.96) + (along[i] * 0.025 - s[i] * 0.125)
        odd = (p[i] * 0.3 - g[i] * 0.25) + force[i][1]
        out[2 * i + 1] = even + odd
        out[2 * i + 2] = even - odd
    planes = (
        (3, axy, rz, vx * jy, g[0], g[1]),
        (5, axz, ry, vx * jz, g[0], g[2]),
        (7, ayz, rx, vy * jz, g[1], g[2]),
    )
    for n, total, across, shear, ga, gb in planes:
        a = (fourth - across * 0.52) - total * 0.075
        b = shear - (s[n] - s[n + 1]) * 0.0625
        e0, e1 = a + b, a - b
        o0, o1 = (ga + gb) - d[n] * 0.3, (ga - gb) - d[n + 1] * 0.3
        out[2 * n + 1], out[2 * n + 2] = e0 + o0, e0 - o0
        out[2 * n + 3], out[2 * n + 4] = e1 + o1, e1 - o1
    return out


def kernel(gy, gz, pop_hbm, mask_hbm, force_hbm, out_ref, raw, raw_mask, force_ref, cells0, cells1, cells2, mask,
           moved_mask, zs, zh, mzs, mzh, load_sem, send_sem, recv_sem):
    state = (cells0, cells1, cells2)
    planes, across = pop_hbm.shape[1], pop_hbm.shape[2] // SEG
    my, mz = lax.axis_index("gy"), lax.axis_index("gz")

    def peer(dy, dz):
        return {"gy": lax.rem(my + dy + gy, gy), "gz": lax.rem(mz + dz + gz, gz)}

    load_mask = pltpu.make_async_copy(mask_hbm, raw_mask, load_sem.at[0])
    load_force = pltpu.make_async_copy(force_hbm, force_ref, load_sem.at[1])
    load_pop = [pltpu.make_async_copy(pop_hbm.at[:, p], raw.at[:, p], load_sem.at[2 + p]) for p in range(planes)]
    load_mask.start()
    load_force.start()
    for copy in load_pop:
        copy.start()
    barrier = pltpu.get_barrier_semaphore()
    for dy, dz in SIDES:
        pl.semaphore_signal(barrier, inc=1, device_id=peer(dy, dz), device_id_type=MESH)

    lane = lax.broadcasted_iota(jnp.int32, (SEG, W), 1)
    line = slice(LO, HI)

    def remote(source, target, number, side):
        return pltpu.make_async_remote_copy(
            src_ref=source,
            dst_ref=target,
            send_sem=send_sem.at[number],
            recv_sem=recv_sem.at[number],
            device_id=peer(*side),
            device_id_type=MESH,
        )

    def edge(dy):
        return (across, 0) if dy == 1 else (1, across + 1)

    def ends(dz):
        return (slice(HI - 1, HI), slice(LO - 1, LO)) if dz == 1 else (slice(LO, LO + 1), slice(HI, HI + 1))

    count = [0]

    def next_sem():
        count[0] += 1
        return count[0] - 1

    def start(group):
        for copy in group:
            copy.start()
        return group

    def arrive(group):
        for copy in group:
            copy.wait_recv()

    sent = []

    def entries(ref, lead):
        return ref.reshape(*lead, across + 2, planes, ROWS, W)

    views = [entries(ref, (19,)) for ref in state]
    mask_view = entries(mask, ())

    def at(y, p, row=LO):
        base = (y * planes + p) * ROWS
        return (base if isinstance(y, int) else pl.multiple_of(base, 8)) + row

    def send_y(buf, dy):
        here, there = edge(dy)
        group = []
        for dz in (1, -1):
            src, dst = ends(dz)
            k = SLOT[velocities.index((0, dy, dz))]
            group.append(remote(views[buf].at[k, here, :, src], views[buf].at[k, there, :, dst], next_sem(), (dy, dz)))
        for a, n in Y_RUN[dy]:
            source, target = views[buf].at[pl.ds(a, n), here, :, line], views[buf].at[pl.ds(a, n), there, :, line]
            group.append(remote(source, target, next_sem(), (dy, 0)))
        sent.append(start(group))
        return group

    def send_z(out, into, lines_of, starts, group):
        copies = []
        for i, dz in enumerate((1, -1)):
            refs = lines_of(dz)
            packed = jnp.zeros((SEG, W), out.dtype)
            row = HI - 1 if dz == 1 else LO
            for j, (load, y) in enumerate((load, y) for load, _ in refs for y in starts):
                shift = (j + 1 if dz == 1 else j) % W
                v = load(pl.ds(at(y, 0, row), SEG, stride=ROWS))
                packed = jnp.where(lane == j, pltpu.roll(v, shift, 1) if shift else v, packed)
            out[group, i] = packed
            copies.append(remote(out.at[group, i], into.at[group, i], next_sem(), (0, dz)))
        sent.append(start(copies))

        def done():
            for i, dz in enumerate((1, -1)):
                copies[i].wait_recv()
                row = LO - 1 if dz == 1 else HI
                packed = into[group, i]
                for j, (store, y) in enumerate((store, y) for _, store in lines_of(dz) for y in starts):
                    shift = (W - 1 - j if dz == 1 else W - j) % W
                    store(pl.ds(at(y, 0, row), SEG, stride=ROWS), pltpu.roll(packed, shift, 1) if shift else packed)

        return done

    def lines_of(ref):
        def pick(dz):
            result = []
            for k in Z_SET[dz]:
                slot = SLOT[k]

                def load(rows, slot=slot):
                    return ref[slot, rows, :]

                def store(rows, value, slot=slot):
                    ref[slot, rows, :] = value

                result.append((load, store))
            return result

        return pick

    def mask_lines(dz):
        def store(rows, value):
            mask[rows, :] = value

        return [(lambda rows: mask[rows, :], store)]

    near_rows, far_rows = [1, across - 1], list(range(3, across - 1, 2))

    def send_state(buf, rows):
        group = buf * 2 + (0 if rows is near_rows else 1)
        return send_z(zs, zh, lines_of(state[buf]), rows, group)

    def send_mask():
        group = []
        for dy in (1, -1):
            here, there = edge(dy)
            for dz in (1, -1):
                src, dst = ends(dz)
                group.append(remote(mask_view.at[here, :, src], mask_view.at[there, :, dst], next_sem(), (dy, dz)))
            group.append(remote(mask_view.at[here, :, line], mask_view.at[there, :, line], next_sem(), (dy, 0)))
        sent.append(start(group))
        return group, send_z(mzs, mzh, mask_lines, near_rows + far_rows, 0)

    def along_z(load, cz):
        v = load(0)
        if cz == 1:
            return pltpu.roll(jnp.where(lane == W - 1, load(-1), v), 1, 1)
        if cz == -1:
            return pltpu.roll(jnp.where(lane == 0, load(1), v), W - 1, 1)
        return v

    def move_mask(y):
        for p in range(planes):
            for i, cz in enumerate((1, -1)):
                moved_mask[i, y, p] = along_z(lambda o: mask[pl.ds(at(y, p, LO + o), SEG), :], cz)

    def streamed(buf, p, y):
        f = []
        for k in range(19):
            cx, cy, cz = velocities[k]
            here = state[buf][SLOT[opposite[k]], pl.ds(at(y, p), SEG), :]
            q = p - cx
            if k == 0 or not 0 <= q < planes:
                f.append(here)
                continue
            moved = along_z(lambda o: state[buf][SLOT[k], pl.ds(at(y - cy, q, LO + o), SEG), :], cz)
            blocked = mask[pl.ds(at(y - cy, q), SEG), :] if cz == 0 else moved_mask[(1 - cz) // 2, y - cy, q]
            f.append(jnp.where(blocked != 0, here, moved))
        return f

    def relax(buf, f, p, y):
        for k, value in enumerate(collide(f, force)):
            state[buf][SLOT[k], pl.ds(at(y, p), SEG), :] = value

    load_mask.wait()
    for p in range(planes):
        for y in range(across):
            mask[pl.ds(at(y + 1, p), SEG), :] = raw_mask[p, pl.ds(y, SEG, stride=across), :]
    load_force.wait()
    force = [(force_ref[i] * (1.0 / 12.0), force_ref[i] * 0.1875) for i in range(3)]

    def first(p, y):
        relax(0, [raw[k, p, pl.ds(y - 1, SEG, stride=across), :] for k in range(19)], p, y)

    for p in range(planes):
        load_pop[p].wait()
        first(p, 1)
        first(p, across)

    pl.semaphore_wait(barrier, len(SIDES))
    coming_mask, mask_done = send_mask()
    coming_y = {dy: send_y(0, dy) for dy in (1, -1)}
    for p in range(planes):
        first(p, 2)
        first(p, across - 1)
    near = send_state(0, near_rows)

    def rest(y, carry):
        for p in range(planes):
            first(p, y)
        return carry

    lax.fori_loop(3, across - 1, rest, 0)
    far = send_state(0, far_rows)

    mask_done()
    arrive(coming_mask)

    def shift(y, carry):
        move_mask(y)
        return carry

    lax.fori_loop(0, across + 2, shift, 0)

    def final(buf, y):
        for p in range(planes):
            rho, jx, jy, jz = moments(streamed(buf, p, y))[-4:]
            fluid = (1 - mask[pl.ds(at(y, p), SEG), :]).astype(jnp.float32)
            scale = fluid * (1.0 / reference_mach) / rho
            spot = pl.ds(y - 1, SEG, stride=across)
            out_ref[0, p, spot, :] = rho * fluid
            out_ref[1, p, spot, :] = jx * scale
            out_ref[2, p, spot, :] = jy * scale
            out_ref[3, p, spot, :] = jz * scale

    def middle(step, y):
        for p in range(planes):
            relax(step + 1, streamed(step, p, y), p, y)

    def interior(block):
        def body(y, carry):
            block(y)
            return carry

        lax.fori_loop(3, across - 1, body, 0)

    for step in range(STEPS - 1):
        near()
        later_y = {}
        for dy, y in ((-1, 1), (1, across)):
            arrive(coming_y[-dy])
            middle(step, y)
            later_y[dy] = send_y(step + 1, dy)
        far()
        middle(step, 2)
        middle(step, across - 1)
        near = send_state(step + 1, near_rows)
        interior(functools.partial(middle, step))
        far = send_state(step + 1, far_rows)
        coming_y = later_y

    last = STEPS - 1
    near()
    far()
    final(last, 2)
    final(last, across - 1)
    interior(functools.partial(final, last))
    for dy, y in ((-1, 1), (1, across)):
        arrive(coming_y[-dy])
        final(last, y)
    for group in sent:
        for copy in group:
            copy.wait_send()


def hand_out(both_ref, den_hbm, vel_hbm, sem):
    den = pltpu.make_async_copy(both_ref.at[0], den_hbm, sem.at[0])
    vel = pltpu.make_async_copy(both_ref.at[pl.ds(1, 3)], vel_hbm, sem.at[1])
    vel.start()
    den.start()
    vel.wait()
    den.wait()


def solution(mesh):
    gy, gz = mesh.shape["gy"], mesh.shape["gz"]

    def tiles(x, across):
        lead = x.shape[:-2]
        x = x.reshape(*lead, across, SEG, W)
        return jnp.swapaxes(x, -3, -2).reshape(*lead, SEG * across, W)

    def lines(x, across):
        lead = x.shape[:-2]
        x = x.reshape(*lead, SEG, across, W)
        return jnp.swapaxes(x, -3, -2).reshape(*lead, across, SEG * W)

    def local(populations, solid_mask, body_force):
        planes, across, length = solid_mask.shape
        if length != SEG * W or across < 6 or across % 2 or 2 * planes != SEG:
            raise ValueError("unsupported block")
        messages = 64
        both = pl.pallas_call(
            functools.partial(kernel, gy, gz),
            out_shape=pltpu.VMEM((4, planes, SEG * across, W), jnp.float32),
            in_specs=[pl.BlockSpec(memory_space=pltpu.HBM)] * 3,
            out_specs=pl.BlockSpec(memory_space=pltpu.VMEM),
            scratch_shapes=[
                pltpu.VMEM((19, planes, SEG * across, W), jnp.float32),
                pltpu.VMEM((planes, SEG * across, W), jnp.int32),
                pltpu.SMEM((3,), jnp.float32),
                *[pltpu.VMEM((19, (across + 2) * planes * ROWS, W), jnp.float32)] * STEPS,
                pltpu.VMEM(((across + 2) * planes * ROWS, W), jnp.int32),
                pltpu.VMEM((2, across + 2, planes, SEG, W), jnp.int32),
                pltpu.VMEM((2 * STEPS, 2, SEG, W), jnp.float32),
                pltpu.VMEM((2 * STEPS, 2, SEG, W), jnp.float32),
                pltpu.VMEM((1, 2, SEG, W), jnp.int32),
                pltpu.VMEM((1, 2, SEG, W), jnp.int32),
                pltpu.SemaphoreType.DMA((2 + planes,)),
                pltpu.SemaphoreType.DMA((messages,)),
                pltpu.SemaphoreType.DMA((messages,)),
            ],
            compiler_params=pltpu.CompilerParams(collective_id=0, has_side_effects=True, vmem_limit_bytes=VMEM_LIMIT),
        )(*[pltpu.with_memory_space_constraint(x, pltpu.HBM) for x in (tiles(populations, across), tiles(solid_mask, across), body_force)])
        density, velocity = pl.pallas_call(
            hand_out,
            out_shape=(
                jax.ShapeDtypeStruct((planes, SEG * across, W), jnp.float32),
                jax.ShapeDtypeStruct((3, planes, SEG * across, W), jnp.float32),
            ),
            in_specs=[pl.BlockSpec(memory_space=pltpu.VMEM)],
            out_specs=(pl.BlockSpec(memory_space=pl.ANY), pl.BlockSpec(memory_space=pl.ANY)),
            scratch_shapes=[pltpu.SemaphoreType.DMA((2,))],
            compiler_params=pltpu.CompilerParams(vmem_limit_bytes=1 << 20),
        )(both)
        return lines(density, across), lines(velocity, across)

    return jax.shard_map(
        local,
        mesh=mesh,
        in_specs=(P(None, None, "gy", "gz"), P(None, "gy", "gz"), P()),
        out_specs=(P(None, "gy", "gz"), P(None, None, "gy", "gz")),
        check_vma=False,
    )
```

```python
import functools

import jax
import jax.numpy as jnp
from jax import lax
from jax.experimental import pallas as pl
from jax.experimental.pallas import tpu as pltpu
from jax.sharding import PartitionSpec as P

STEPS = 3
W = 128
SEG = 8
VMEM_LIMIT = 60 << 20
LO, HI, ROWS = 8, 16, 24
DEEP, STRIP, SPARE = 2, 3, 5

velocities = [
    (0, 0, 0),
    (1, 0, 0),
    (-1, 0, 0),
    (0, 1, 0),
    (0, -1, 0),
    (0, 0, 1),
    (0, 0, -1),
    (1, 1, 0),
    (-1, -1, 0),
    (1, -1, 0),
    (-1, 1, 0),
    (1, 0, 1),
    (-1, 0, -1),
    (1, 0, -1),
    (-1, 0, 1),
    (0, 1, 1),
    (0, -1, -1),
    (0, 1, -1),
    (0, -1, 1),
]
opposite = [0, 2, 1, 4, 3, 6, 5, 8, 7, 10, 9, 12, 11, 14, 13, 16, 15, 18, 17]
reference_mach = 0.05
ORDER = [5, 11, 14, 15, 3, 7, 10, 17, 6, 12, 13, 16, 4, 8, 9, 18, 0, 1, 2]
SLOT = [ORDER.index(k) for k in range(19)]
Y_RUN = {1: (3, 5), -1: (11, 5)}
Y_SET = {dy: [k for k in ORDER if velocities[k][1] == dy] for dy in (1, -1)}
PART = {dy: [k for k in ORDER if velocities[k][1] != -dy] for dy in (1, -1)}
SIDES = [(1, 0), (-1, 0), (0, 1), (0, -1)]
MESH = pl.DeviceIdType.MESH


def moments(f):
    s = [f[2 * a + 1] + f[2 * a + 2] for a in range(9)]
    d = [f[2 * a + 1] - f[2 * a + 2] for a in range(9)]
    axes = s[0] + s[1] + s[2]
    a = (s[3] + s[4], s[5] + s[6], s[7] + s[8])
    edges = a[0] + a[1] + a[2]
    rho = f[0] + axes + edges
    px, py, pz = (d[3] + d[4]) + (d[5] + d[6]), (d[3] - d[4]) + (d[7] + d[8]), (d[5] - d[6]) + (d[7] - d[8])
    jx, jy, jz = d[0] + px, d[1] + py, d[2] + pz
    return s, d, a, (axes, edges), (px, py, pz), rho, jx, jy, jz


def collide(f, force):
    s, d, (axy, axz, ayz), (axes, edges), p, rho, jx, jy, jz = moments(f)
    w = 0.3125 / rho
    vx, vy, vz = jx * w, jy * w, jz * w
    rx, ry, rz = jx * vx, jy * vy, jz * vz
    r = rx + ry + rz
    r3 = r * (0.325 / 0.9375)
    common = rho * (0.625 / 3.0 - 1.3 / 9.0) - r3
    fourth = rho * (0.325 / 9.0) + r3
    out = [None] * 19
    out[0] = (rho * (1.3 / 3.0 - 0.25) - r * 1.92) + (axes * 0.25 + edges * 0.2)
    g = [j * (0.4 / 3.0) + force[i][0] for i, j in enumerate((jx, jy, jz))]
    along = (axy + axz, axy + ayz, axz + ayz)
    for i, ri in enumerate((rx, ry, rz)):
        even = (common + ri * 0.96) + (along[i] * 0.025 - s[i] * 0.125)
        odd = (p[i] * 0.3 - g[i] * 0.25) + force[i][1]
        out[2 * i + 1] = even + odd
        out[2 * i + 2] = even - odd
    planes = (
        (3, axy, rz, vx * jy, g[0], g[1]),
        (5, axz, ry, vx * jz, g[0], g[2]),
        (7, ayz, rx, vy * jz, g[1], g[2]),
    )
    for n, total, across, shear, ga, gb in planes:
        a = (fourth - across * 0.52) - total * 0.075
        b = shear - (s[n] - s[n + 1]) * 0.0625
        e0, e1 = a + b, a - b
        o0, o1 = (ga + gb) - d[n] * 0.3, (ga - gb) - d[n + 1] * 0.3
        out[2 * n + 1], out[2 * n + 2] = e0 + o0, e0 - o0
        out[2 * n + 3], out[2 * n + 4] = e1 + o1, e1 - o1
    return out


def kernel(gy, gz, pop_hbm, mask_hbm, force_hbm, out_ref, raw, raw_mask, force_ref, cells0, cells1, cells2, strip0, strip1,
           mask, moved_mask, strip_mask, strip_flag, zs, zh, mzs, mzh, part, part_h, spart, spart_h, third, third_h,
           load_sem, send_sem, recv_sem):
    state, strips = (cells0, cells1, cells2), (strip0, strip1)
    planes, across = pop_hbm.shape[1], pop_hbm.shape[2] // SEG
    total = across + 2 * DEEP
    my, mz = lax.axis_index("gy"), lax.axis_index("gz")

    def peer(dy, dz):
        return {"gy": lax.rem(my + dy + gy, gy), "gz": lax.rem(mz + dz + gz, gz)}

    load_mask = pltpu.make_async_copy(mask_hbm, raw_mask, load_sem.at[0])
    load_force = pltpu.make_async_copy(force_hbm, force_ref, load_sem.at[1])
    load_pop = [pltpu.make_async_copy(pop_hbm.at[:, p], raw.at[:, p], load_sem.at[2 + p]) for p in range(planes)]
    load_mask.start()
    load_force.start()
    for copy in load_pop:
        copy.start()
    barrier = pltpu.get_barrier_semaphore()
    for dy, dz in SIDES:
        pl.semaphore_signal(barrier, inc=1, device_id=peer(dy, dz), device_id_type=MESH)

    lane = lax.broadcasted_iota(jnp.int32, (SEG, W), 1)
    plane_of = lax.rem(lax.broadcasted_iota(jnp.int32, (SEG, W), 0), planes)
    triple = (lane * 43) >> 7
    line = slice(LO, HI)
    count = [0]
    sent = []

    def send(source, target, side):
        copy = pltpu.make_async_remote_copy(
            src_ref=source,
            dst_ref=target,
            send_sem=send_sem.at[count[0]],
            recv_sem=recv_sem.at[count[0]],
            device_id=peer(*side),
            device_id_type=MESH,
        )
        count[0] += 1
        copy.start()
        sent.append(copy)
        return copy

    def arrive(copies):
        for copy in copies:
            copy.wait_recv()

    def view(ref, lead):
        return ref.reshape(*lead, total * planes + 2 * SPARE, ROWS, W)

    views = [view(ref, (19,)) for ref in state]
    mask_view = view(mask, ())

    def at(y, p, row=LO):
        return ((y * planes + p) + SPARE) * ROWS + row

    def lines(y, n=1):
        return pl.ds(y * planes + SPARE, n * planes)

    def spot(y):
        return SEG + y * planes

    low, high = DEEP, across + DEEP - 1
    EDGE = {1: (high, low - 1), -1: (low, high + 1)}
    BEHIND = {1: (high - 1, low - 2), -1: (low + 1, high + 2)}
    own_pairs = list(range(DEEP, DEEP + across, 2))
    all_pairs = list(range(0, total, 2))

    def pair_of(y):
        return y - y % 2

    def along_z(load, cz):
        v = load(0)
        if cz == 1:
            return pltpu.roll(jnp.where(lane == W - 1, load(-1), v), 1, 1)
        if cz == -1:
            return pltpu.roll(jnp.where(lane == 0, load(1), v), W - 1, 1)
        return v

    def move_mask(y):
        for p in range(planes):
            for i, cz in enumerate((1, -1)):
                moved_mask[i, y, p] = along_z(lambda o: mask[pl.ds(at(y, p, LO + o), SEG), :], cz)

    def streamed(step, p, y, ks=range(19)):
        f = {}
        for k in ks:
            cx, cy, cz = velocities[k]
            here = state[step][SLOT[opposite[k]], pl.ds(at(y, p), SEG), :]
            q = p - cx
            if k == 0 or not 0 <= q < planes:
                f[k] = here
                continue
            moved = along_z(lambda o: state[step][SLOT[k], pl.ds(at(y - cy, q, LO + o), SEG), :], cz)
            blocked = mask[pl.ds(at(y - cy, q), SEG), :] if cz == 0 else moved_mask[(1 - cz) // 2, y - cy, q]
            f[k] = jnp.where(blocked != 0, here, moved)
        return f

    def relax(step, f, p, y, ks=range(19)):
        out = collide(f, force)
        for k in ks:
            state[step][SLOT[k], pl.ds(at(y, p), SEG), :] = out[k]

    def advance(step, y):
        for p in range(planes):
            relax(step, streamed(step - 1, p, y), p, y)

    def final(y):
        for p in range(planes):
            rho, jx, jy, jz = moments(streamed(STEPS - 1, p, y))[-4:]
            fluid = (1 - mask[pl.ds(at(y, p), SEG), :]).astype(jnp.float32)
            scale = fluid * (1.0 / reference_mach) / rho
            rows = pl.ds(y - DEEP, SEG, stride=across)
            out_ref[0, p, rows, :] = rho * fluid
            out_ref[1, p, rows, :] = jx * scale
            out_ref[2, p, rows, :] = jy * scale
            out_ref[3, p, rows, :] = jz * scale

    def strip_rows(y):
        return pl.ds(spot(y), SEG)

    def every_line(y, row):
        return pl.ds(at(y, 0, row), SEG, stride=ROWS)

    def strip_move(ref_strip, ref_lines, y, c):
        cx, cy, cz = c
        v = ref_strip(strip_rows(y - cy))
        if cz == 1:
            v = pltpu.roll(jnp.where(lane == W - 1, ref_lines(every_line(y - cy, HI - 1)), v), 1, 1)
        elif cz == -1:
            v = pltpu.roll(jnp.where(lane == 0, ref_lines(every_line(y - cy, LO)), v), W - 1, 1)
        return pltpu.roll(v, cx % SEG, 0) if cx else v

    def flag_strip(y, ks=range(19)):
        for k in ks:
            cx = velocities[k][0]
            if k == 0:
                continue
            v = strip_move(lambda rows: strip_mask[rows, :], lambda rows: mask[rows, :], y, velocities[k])
            if cx:
                v = jnp.where(plane_of == (0 if cx == 1 else planes - 1), 1, v)
            strip_flag[k, y] = v

    def strip_streamed(step, y, ks=range(19)):
        f = {}
        for k in ks:
            slot = SLOT[k]
            here = strips[step][SLOT[opposite[k]], strip_rows(y), :]
            if k == 0:
                f[k] = here
                continue
            moved = strip_move(
                lambda rows: strips[step][slot, rows, :], lambda rows: state[step][slot, rows, :], y, velocities[k]
            )
            f[k] = jnp.where(strip_flag[k, y] != 0, here, moved)
        return f

    def attach(ref, k, y, value):
        cz = velocities[k][2]
        if cz:
            ref[SLOT[k], every_line(y, LO - 1 if cz == 1 else HI), :] = value

    def strip_relax(step, f, y):
        out = collide(f, force)
        for k in range(19):
            if step < STEPS - 1:
                strips[step][SLOT[k], strip_rows(y), :] = out[k]
            attach(state[step], k, y, out[k])

    def strip_advance(step, y):
        strip_relax(step, strip_streamed(step - 1, y), y)

    load_mask.wait()
    for p in range(planes):
        for y in range(across):
            mask[pl.ds(at(y + DEEP, p), SEG), :] = raw_mask[p, pl.ds(y, SEG, stride=across), :]
    load_force.wait()
    force = [(force_ref[i] * (1.0 / 12.0), force_ref[i] * 0.1875) for i in range(3)]
    group = max(u for u in (4, 2, 1) if across % u == 0)
    for p in range(planes):
        load_pop[p].wait()

        def first(i, carry, p=p):
            for n in range(group):
                y = i * group + n
                f = [raw[k, p, pl.ds(y, SEG, stride=across), :] for k in range(19)]
                base = pl.multiple_of(at(y + DEEP, p), 8)
                for k, value in enumerate(collide(f, force)):
                    state[0][SLOT[k], pl.ds(base, SEG), :] = value
            return carry

        lax.fori_loop(0, across // group, first, 0)

    groups = [(y, k) for y in own_pairs for k in range(19)]
    per_tile = W // STRIP

    def pack(out, tile, i, loads):
        row = HI - 1 if i == 0 else LO
        packed = jnp.zeros((SEG, W), out.dtype)
        for j, load in enumerate(loads):
            shift = (STRIP * j + (STRIP if i == 0 else 0)) % W
            v = load(row)
            packed = jnp.where(triple == j, pltpu.roll(v, shift, 1) if shift else v, packed)
        out[i, tile] = packed

    def unpack(into, tile, j):
        left, right = into[0, tile], into[1, tile]
        a, b = (W - STRIP - STRIP * j) % W, (W - STRIP * j) % W
        left = pltpu.roll(left, a, 1) if a else left
        right = pltpu.roll(right, b, 1) if b else right
        return jnp.where(lane < W // 2, right, left)

    tiles = [groups[n : n + per_tile] for n in range(0, len(groups), per_tile)]
    for i in range(2):
        pack(mzs, 0, i, [lambda row, y=y: mask[every_line(y, row), :] for y in own_pairs])
        for t, tile in enumerate(tiles):
            pack(zs, t, i, [lambda row, y=y, k=k: state[0][SLOT[k], every_line(y, row), :] for y, k in tile])

    pl.semaphore_wait(barrier, len(SIDES))
    coming_z = []
    for i, dz in enumerate((1, -1)):
        coming_z.append(send(mzs.at[i], mzh.at[i], (0, dz)))
        coming_z.append(send(zs.at[i], zh.at[i], (0, dz)))
    coming_mask, coming1, coming2, coming3 = [], [], [], []
    for dy in (1, -1):
        here, there = min(EDGE[dy][0], BEHIND[dy][0]), min(EDGE[dy][1], BEHIND[dy][1])
        coming_mask.append(send(mask_view.at[lines(here, 2), line], mask_view.at[lines(there, 2), line], (dy, 0)))
    for dy in (1, -1):
        (here, there), run = EDGE[dy], pl.ds(*Y_RUN[dy])
        coming1.append(send(views[0].at[run, lines(here), line], views[0].at[run, lines(there), line], (dy, 0)))

    arrive(coming_z)
    for j, y in enumerate(own_pairs):
        value = unpack(mzh, 0, j)
        strip_mask[strip_rows(y), :] = value
        mask[every_line(y, LO - 1), :] = value
        mask[every_line(y, HI), :] = value
    for t, tile in enumerate(tiles):
        for j, (y, k) in enumerate(tile):
            value = unpack(zh, t, j)
            strip0[SLOT[k], strip_rows(y), :] = value
            attach(cells0, k, y, value)
    for y in range(low, high + 1):
        move_mask(y)
    for dy in (1, -1):
        flag_strip(pair_of(EDGE[dy][0]), PART[dy])

    def half(dy):
        return (slice(planes, 2 * planes), slice(0, planes)) if dy == 1 else (slice(0, planes), slice(planes, 2 * planes))

    for i, dy in enumerate((1, -1)):
        here, there = EDGE[dy]
        run = pl.ds(*Y_RUN[dy])
        for p in range(planes):
            f = streamed(0, p, here, PART[dy])
            for n, k in enumerate(PART[dy]):
                part[i, n, p] = f[k]
        coming2.append(send(part.at[i], part_h.at[i], (dy, 0)))
    for i, dy in enumerate((1, -1)):
        here, there = EDGE[dy]
        run = pl.ds(*Y_RUN[dy])
        f = strip_streamed(0, pair_of(here), PART[dy])
        for n, k in enumerate(PART[dy]):
            spart[i, n] = f[k]
        coming2.append(send(spart.at[i, :, half(dy)[0]], spart_h.at[i, :, half(dy)[0]], (dy, 0)))
        coming1.append(send(strip0.at[run, pl.ds(spot(here), planes)], strip0.at[run, pl.ds(spot(there), planes)], (dy, 0)))
        a, b = pair_of(here), pair_of(there)
        coming_mask.append(send(strip_mask.at[strip_rows(a)], strip_mask.at[strip_rows(b)], (dy, 0)))
    for i, dy in enumerate((1, -1)):
        here, there = BEHIND[dy]
        run = pl.ds(*Y_RUN[dy])
        advance(1, here)
        coming3.append(send(views[1].at[run, lines(here), line], views[1].at[run, lines(there), line], (dy, 0)))
    for y in range(low + 1, high, 2):
        flag_strip(y)
        strip_advance(1, y)
    for i, dy in enumerate((1, -1)):
        here, there = BEHIND[dy]
        for n, k in enumerate(Y_SET[dy]):
            third[i, n] = strip1[SLOT[k], strip_rows(pair_of(here)), :]
        coming3.append(send(third.at[i, :, half(dy)[1]], third_h.at[i, :, half(dy)[1]], (dy, 0)))

    def over(first_row, last_row, block):
        def body(y, carry):
            block(y)
            return carry

        lax.fori_loop(first_row, last_row + 1, body, 0)

    over(low + 2, high - 2, functools.partial(advance, 1))
    over(low + 2, high - 2, functools.partial(advance, 2))
    for y in own_pairs[1:-1]:
        flag_strip(y)
        strip_advance(2, y)
    over(low + 3, high - 3, final)

    arrive(coming_mask)
    for dy in (1, -1):
        y = pair_of(EDGE[dy][1])
        value = strip_mask[strip_rows(y), :]
        mask[every_line(y, LO - 1), :] = value
        mask[every_line(y, HI), :] = value
        for there in (EDGE[dy][1], BEHIND[dy][1]):
            move_mask(there)
    for y in all_pairs:
        if y not in own_pairs[1:-1]:
            flag_strip(y)
    arrive(coming1)
    for dy in (1, -1):
        y = pair_of(EDGE[dy][1])
        for k in Y_SET[dy]:
            attach(cells0, k, y, strip0[SLOT[k], strip_rows(y), :])

    def finish(halves, i, dy, y):
        for p in range(planes):
            f = streamed(0, p, y, Y_SET[-dy])
            f.update({k: halves[i, n, p] for n, k in enumerate(PART[dy])})
            relax(1, f, p, y)

    for i, dy in enumerate((1, -1)):
        finish(part, i, dy, EDGE[dy][0])
        strip_advance(1, pair_of(EDGE[dy][0]))
    for dy in (1, -1):
        advance(2, BEHIND[dy][0])

    arrive(coming2)
    for i, dy in enumerate((1, -1)):
        y = EDGE[dy][1]
        finish(part_h, i, dy, y)
        y = pair_of(y)
        f = strip_streamed(0, y, Y_SET[-dy])
        f.update({k: spart_h[i, n] for n, k in enumerate(PART[dy])})
        strip_relax(1, f, y)
    for dy in (1, -1):
        advance(2, EDGE[dy][0])
        strip_advance(2, pair_of(EDGE[dy][0]))
    for y in (low + 1, low + 2, high - 2, high - 1):
        final(y)

    arrive(coming3)
    for i, dy in enumerate((1, -1)):
        y, behind = EDGE[dy][1], BEHIND[dy][1]
        pair = pair_of(y)
        for n, k in enumerate(Y_SET[dy]):
            strip1[SLOT[k], pl.ds(spot(behind), planes), :] = third_h[i, n, half(dy)[1], :]
            if velocities[k][2]:
                attach(cells1, k, pair, strip1[SLOT[k], strip_rows(pair), :])
        for p in range(planes):
            relax(2, streamed(1, p, y), p, y, Y_SET[dy])
        strip_advance(2, pair)
        final(low if dy == 1 else high)
    for copy in sent:
        copy.wait_send()


def hand_out(both_ref, den_hbm, vel_hbm, sem):
    den = pltpu.make_async_copy(both_ref.at[0], den_hbm, sem.at[0])
    vel = pltpu.make_async_copy(both_ref.at[pl.ds(1, 3)], vel_hbm, sem.at[1])
    vel.start()
    den.start()
    vel.wait()
    den.wait()


def solution(mesh):
    gy, gz = mesh.shape["gy"], mesh.shape["gz"]

    def tiles(x, across):
        lead = x.shape[:-2]
        x = x.reshape(*lead, across, SEG, W)
        return jnp.swapaxes(x, -3, -2).reshape(*lead, SEG * across, W)

    def lines(x, across):
        lead = x.shape[:-2]
        x = x.reshape(*lead, SEG, across, W)
        return jnp.swapaxes(x, -3, -2).reshape(*lead, across, SEG * W)

    def local(populations, solid_mask, body_force):
        planes, across, length = solid_mask.shape
        if length != SEG * W or across < 8 or across % 2 or 2 * planes != SEG:
            raise ValueError("unsupported block")
        messages = 32
        total = across + 2 * DEEP
        entries = (total * planes + 2 * SPARE) * ROWS
        strip = total * planes + 2 * SEG
        packs = -(-19 * (across // 2) // (W // STRIP))
        both = pl.pallas_call(
            functools.partial(kernel, gy, gz),
            out_shape=pltpu.VMEM((4, planes, SEG * across, W), jnp.float32),
            in_specs=[pl.BlockSpec(memory_space=pltpu.HBM)] * 3,
            out_specs=pl.BlockSpec(memory_space=pltpu.VMEM),
            scratch_shapes=[
                pltpu.VMEM((19, planes, SEG * across, W), jnp.float32),
                pltpu.VMEM((planes, SEG * across, W), jnp.int32),
                pltpu.SMEM((3,), jnp.float32),
                *[pltpu.VMEM((19, entries, W), jnp.float32)] * STEPS,
                *[pltpu.VMEM((19, strip, W), jnp.float32)] * (STEPS - 1),
                pltpu.VMEM((entries, W), jnp.int32),
                pltpu.VMEM((2, total, planes, SEG, W), jnp.int32),
                pltpu.VMEM((strip, W), jnp.int32),
                pltpu.VMEM((19, total, SEG, W), jnp.int32),
                *[pltpu.VMEM((2, packs, SEG, W), jnp.float32)] * 2,
                *[pltpu.VMEM((2, 1, SEG, W), jnp.int32)] * 2,
                *[pltpu.VMEM((2, 14, planes, SEG, W), jnp.float32)] * 2,
                *[pltpu.VMEM((2, 14, SEG, W), jnp.float32)] * 2,
                *[pltpu.VMEM((2, 5, SEG, W), jnp.float32)] * 2,
                pltpu.SemaphoreType.DMA((2 + planes,)),
                pltpu.SemaphoreType.DMA((messages,)),
                pltpu.SemaphoreType.DMA((messages,)),
            ],
            compiler_params=pltpu.CompilerParams(collective_id=0, has_side_effects=True, vmem_limit_bytes=VMEM_LIMIT),
        )(*[pltpu.with_memory_space_constraint(x, pltpu.HBM) for x in (tiles(populations, across), tiles(solid_mask, across), body_force)])
        density, velocity = pl.pallas_call(
            hand_out,
            out_shape=(
                jax.ShapeDtypeStruct((planes, SEG * across, W), jnp.float32),
                jax.ShapeDtypeStruct((3, planes, SEG * across, W), jnp.float32),
            ),
            in_specs=[pl.BlockSpec(memory_space=pltpu.VMEM)],
            out_specs=(pl.BlockSpec(memory_space=pl.ANY), pl.BlockSpec(memory_space=pl.ANY)),
            scratch_shapes=[pltpu.SemaphoreType.DMA((2,))],
            compiler_params=pltpu.CompilerParams(vmem_limit_bytes=1 << 20),
        )(both)
        return lines(density, across), lines(velocity, across)

    return jax.shard_map(
        local,
        mesh=mesh,
        in_specs=(P(None, None, "gy", "gz"), P(None, "gy", "gz"), P()),
        out_specs=(P(None, "gy", "gz"), P(None, None, "gy", "gz")),
        check_vma=False,
    )
```

```python
import functools

import jax
import jax.numpy as jnp
from jax import lax
from jax.experimental import pallas as pl
from jax.experimental.pallas import tpu as pltpu
from jax.sharding import PartitionSpec as P

STEPS = 3
W = 128
SEG = 8
VMEM_LIMIT = 60 << 20
LO, HI, ROWS = 8, 16, 24
DEEP, STRIP, SPARE = 2, 3, 5

velocities = [
    (0, 0, 0),
    (1, 0, 0),
    (-1, 0, 0),
    (0, 1, 0),
    (0, -1, 0),
    (0, 0, 1),
    (0, 0, -1),
    (1, 1, 0),
    (-1, -1, 0),
    (1, -1, 0),
    (-1, 1, 0),
    (1, 0, 1),
    (-1, 0, -1),
    (1, 0, -1),
    (-1, 0, 1),
    (0, 1, 1),
    (0, -1, -1),
    (0, 1, -1),
    (0, -1, 1),
]
opposite = [0, 2, 1, 4, 3, 6, 5, 8, 7, 10, 9, 12, 11, 14, 13, 16, 15, 18, 17]
reference_mach = 0.05
ORDER = [5, 11, 14, 15, 3, 7, 10, 17, 6, 12, 13, 16, 4, 8, 9, 18, 0, 1, 2]
SLOT = [ORDER.index(k) for k in range(19)]
Y_RUN = {1: (3, 5), -1: (11, 5)}
Y_SET = {dy: [k for k in ORDER if velocities[k][1] == dy] for dy in (1, -1)}
PART = {dy: [k for k in ORDER if velocities[k][1] != -dy] for dy in (1, -1)}
SIDES = [(1, 0), (-1, 0), (0, 1), (0, -1)]
MESH = pl.DeviceIdType.MESH


def moments(f):
    s = [f[2 * a + 1] + f[2 * a + 2] for a in range(9)]
    d = [f[2 * a + 1] - f[2 * a + 2] for a in range(9)]
    axes = s[0] + s[1] + s[2]
    a = (s[3] + s[4], s[5] + s[6], s[7] + s[8])
    edges = a[0] + a[1] + a[2]
    rho = f[0] + axes + edges
    px, py, pz = (d[3] + d[4]) + (d[5] + d[6]), (d[3] - d[4]) + (d[7] + d[8]), (d[5] - d[6]) + (d[7] - d[8])
    jx, jy, jz = d[0] + px, d[1] + py, d[2] + pz
    return s, d, a, (axes, edges), (px, py, pz), rho, jx, jy, jz


def collide(f, force):
    s, d, (axy, axz, ayz), (axes, edges), p, rho, jx, jy, jz = moments(f)
    w = 0.3125 / rho
    vx, vy, vz = jx * w, jy * w, jz * w
    rx, ry, rz = jx * vx, jy * vy, jz * vz
    r = rx + ry + rz
    r3 = r * (0.325 / 0.9375)
    common = rho * (0.625 / 3.0 - 1.3 / 9.0) - r3
    fourth = rho * (0.325 / 9.0) + r3
    out = [None] * 19
    out[0] = (rho * (1.3 / 3.0 - 0.25) - r * 1.92) + (axes * 0.25 + edges * 0.2)
    g = [j * (0.4 / 3.0) + force[i][0] for i, j in enumerate((jx, jy, jz))]
    along = (axy + axz, axy + ayz, axz + ayz)
    for i, ri in enumerate((rx, ry, rz)):
        even = (common + ri * 0.96) + (along[i] * 0.025 - s[i] * 0.125)
        odd = (p[i] * 0.3 - g[i] * 0.25) + force[i][1]
        out[2 * i + 1] = even + odd
        out[2 * i + 2] = even - odd
    planes = (
        (3, axy, rz, vx * jy, g[0], g[1]),
        (5, axz, ry, vx * jz, g[0], g[2]),
        (7, ayz, rx, vy * jz, g[1], g[2]),
    )
    for n, total, across, shear, ga, gb in planes:
        a = (fourth - across * 0.52) - total * 0.075
        b = shear - (s[n] - s[n + 1]) * 0.0625
        e0, e1 = a + b, a - b
        o0, o1 = (ga + gb) - d[n] * 0.3, (ga - gb) - d[n + 1] * 0.3
        out[2 * n + 1], out[2 * n + 2] = e0 + o0, e0 - o0
        out[2 * n + 3], out[2 * n + 4] = e1 + o1, e1 - o1
    return out


def kernel(gy, gz, pop_hbm, mask_hbm, force_hbm, out_ref, raw, raw_mask, force_ref, cells0, cells1, cells2, strip0, strip1,
           mask, moved_mask, strip_mask, strip_flag, zs, zh, mzs, mzh, part_e, part, part_h, third_e, spart, spart_h,
           third, third_h,
           load_sem, send_sem, recv_sem):
    state, strips = (cells0, cells1, cells2), (strip0, strip1)
    planes, across = pop_hbm.shape[1], pop_hbm.shape[2] // SEG
    total = across + 2 * DEEP
    my, mz = lax.axis_index("gy"), lax.axis_index("gz")

    def peer(dy, dz):
        return {"gy": lax.rem(my + dy + gy, gy), "gz": lax.rem(mz + dz + gz, gz)}

    load_mask = pltpu.make_async_copy(mask_hbm, raw_mask, load_sem.at[0])
    load_force = pltpu.make_async_copy(force_hbm, force_ref, load_sem.at[1])
    load_pop = [pltpu.make_async_copy(pop_hbm.at[:, p], raw.at[:, p], load_sem.at[2 + p]) for p in range(planes)]
    load_mask.start()
    load_force.start()
    for copy in load_pop:
        copy.start()
    barrier = pltpu.get_barrier_semaphore()
    for dy, dz in SIDES:
        pl.semaphore_signal(barrier, inc=1, device_id=peer(dy, dz), device_id_type=MESH)

    lane = lax.broadcasted_iota(jnp.int32, (SEG, W), 1)
    plane_of = lax.rem(lax.broadcasted_iota(jnp.int32, (SEG, W), 0), planes)
    triple = (lane * 43) >> 7
    line = slice(LO, HI)
    count = [0]
    sent = []

    def send(source, target, side):
        copy = pltpu.make_async_remote_copy(
            src_ref=source,
            dst_ref=target,
            send_sem=send_sem.at[count[0]],
            recv_sem=recv_sem.at[count[0]],
            device_id=peer(*side),
            device_id_type=MESH,
        )
        count[0] += 1
        copy.start()
        sent.append(copy)
        return copy

    def arrive(copies):
        for copy in copies:
            copy.wait_recv()

    def view(ref, lead):
        return ref.reshape(*lead, total * planes + 2 * SPARE, ROWS, W)

    views = [view(ref, (19,)) for ref in state]
    mask_view = view(mask, ())

    def at(y, p, row=LO):
        return ((y * planes + p) + SPARE) * ROWS + row

    def lines(y, n=1):
        return pl.ds(y * planes + SPARE, n * planes)

    def spot(y):
        return SEG + y * planes

    low, high = DEEP, across + DEEP - 1
    EDGE = {1: (high, low - 1), -1: (low, high + 1)}
    BEHIND = {1: (high - 1, low - 2), -1: (low + 1, high + 2)}
    own_pairs = list(range(DEEP, DEEP + across, 2))
    all_pairs = list(range(0, total, 2))

    def pair_of(y):
        return y - y % 2

    def along_z(load, cz):
        v = load(0)
        if cz == 1:
            return pltpu.roll(jnp.where(lane == W - 1, load(-1), v), 1, 1)
        if cz == -1:
            return pltpu.roll(jnp.where(lane == 0, load(1), v), W - 1, 1)
        return v

    def move_mask(y):
        for p in range(planes):
            for i, cz in enumerate((1, -1)):
                moved_mask[i, y, p] = along_z(lambda o: mask[pl.ds(at(y, p, LO + o), SEG), :], cz)

    def streamed(step, p, y, ks=range(19)):
        f = {}
        for k in ks:
            cx, cy, cz = velocities[k]
            here = state[step][SLOT[opposite[k]], pl.ds(at(y, p), SEG), :]
            q = p - cx
            if k == 0 or not 0 <= q < planes:
                f[k] = here
                continue
            moved = along_z(lambda o: state[step][SLOT[k], pl.ds(at(y - cy, q, LO + o), SEG), :], cz)
            blocked = mask[pl.ds(at(y - cy, q), SEG), :] if cz == 0 else moved_mask[(1 - cz) // 2, y - cy, q]
            f[k] = jnp.where(blocked != 0, here, moved)
        return f

    def relax(step, f, p, y, ks=range(19)):
        out = collide(f, force)
        for k in ks:
            state[step][SLOT[k], pl.ds(at(y, p), SEG), :] = out[k]

    def advance(step, y):
        for p in range(planes):
            relax(step, streamed(step - 1, p, y), p, y)

    def final(y):
        for p in range(planes):
            rho, jx, jy, jz = moments(streamed(STEPS - 1, p, y))[-4:]
            fluid = (1 - mask[pl.ds(at(y, p), SEG), :]).astype(jnp.float32)
            scale = fluid * (1.0 / reference_mach) / rho
            rows = pl.ds(y - DEEP, SEG, stride=across)
            out_ref[0, p, rows, :] = rho * fluid
            out_ref[1, p, rows, :] = jx * scale
            out_ref[2, p, rows, :] = jy * scale
            out_ref[3, p, rows, :] = jz * scale

    def strip_rows(y):
        return pl.ds(spot(y), SEG)

    def every_line(y, row):
        return pl.ds(at(y, 0, row), SEG, stride=ROWS)

    def strip_move(ref_strip, ref_lines, y, c):
        cx, cy, cz = c
        v = ref_strip(strip_rows(y - cy))
        if cz == 1:
            v = pltpu.roll(jnp.where(lane == W - 1, ref_lines(every_line(y - cy, HI - 1)), v), 1, 1)
        elif cz == -1:
            v = pltpu.roll(jnp.where(lane == 0, ref_lines(every_line(y - cy, LO)), v), W - 1, 1)
        return pltpu.roll(v, cx % SEG, 0) if cx else v

    def flag_strip(y, ks=range(19)):
        for k in ks:
            cx = velocities[k][0]
            if k == 0:
                continue
            v = strip_move(lambda rows: strip_mask[rows, :], lambda rows: mask[rows, :], y, velocities[k])
            if cx:
                v = jnp.where(plane_of == (0 if cx == 1 else planes - 1), 1, v)
            strip_flag[k, y] = v

    def strip_streamed(step, y, ks=range(19)):
        f = {}
        for k in ks:
            slot = SLOT[k]
            here = strips[step][SLOT[opposite[k]], strip_rows(y), :]
            if k == 0:
                f[k] = here
                continue
            moved = strip_move(
                lambda rows: strips[step][slot, rows, :], lambda rows: state[step][slot, rows, :], y, velocities[k]
            )
            f[k] = jnp.where(strip_flag[k, y] != 0, here, moved)
        return f

    def attach(ref, k, y, value):
        cz = velocities[k][2]
        if cz:
            ref[SLOT[k], every_line(y, LO - 1 if cz == 1 else HI), :] = value

    def strip_relax(step, f, y):
        out = collide(f, force)
        for k in range(19):
            if step < STEPS - 1:
                strips[step][SLOT[k], strip_rows(y), :] = out[k]
            attach(state[step], k, y, out[k])

    def strip_advance(step, y):
        strip_relax(step, strip_streamed(step - 1, y), y)

    load_mask.wait()
    for p in range(planes):
        for y in range(across):
            mask[pl.ds(at(y + DEEP, p), SEG), :] = raw_mask[p, pl.ds(y, SEG, stride=across), :]
    load_force.wait()
    force = [(force_ref[i] * (1.0 / 12.0), force_ref[i] * 0.1875) for i in range(3)]

    def first(p, y):
        f = [raw[k, p, pl.ds(y - DEEP, SEG, stride=across), :] for k in range(19)]
        for k, value in enumerate(collide(f, force)):
            state[0][SLOT[k], pl.ds(at(y, p), SEG), :] = value

    def first_rows(*rows):
        for y in rows:
            for p in range(planes):
                first(p, y)

    for p in range(planes):
        load_pop[p].wait()
        first(p, low)
        first(p, high)

    groups = [(p, k) for p in range(planes) for k in range(19)]
    per_tile = W // STRIP

    def pack(out, tile, i, loads):
        end = pl.ds((SEG - 1) * across, across) if i == 0 else pl.ds(0, across)
        packed = jnp.zeros((SEG, W), out.dtype)
        for j, load in enumerate(loads):
            shift = (STRIP * j + (STRIP if i == 0 else 0)) % W
            v = load(end)
            packed = jnp.where(triple == j, pltpu.roll(v, shift, 1) if shift else v, packed)
        out[i, tile] = packed

    def unpack(into, tile, j):
        left, right = into[0, tile], into[1, tile]
        a, b = (W - STRIP - STRIP * j) % W, (W - STRIP * j) % W
        left = pltpu.roll(left, a, 1) if a else left
        right = pltpu.roll(right, b, 1) if b else right
        return jnp.where(lane < W // 2, right, left)

    tiles = [groups[n : n + per_tile] for n in range(0, len(groups), per_tile)]
    for i in range(2):
        pack(mzs, 0, i, [lambda end, p=p: raw_mask[p, end, :] for p in range(planes)])
        for t, tile in enumerate(tiles):
            pack(zs, t, i, [lambda end, p=p, k=k: raw[k, p, end, :] for p, k in tile])

    pl.semaphore_wait(barrier, len(SIDES))
    coming_z = []
    for i, dz in enumerate((1, -1)):
        coming_z.append(send(mzs.at[i], mzh.at[i], (0, dz)))
        coming_z.append(send(zs.at[i], zh.at[i], (0, dz)))
    coming_mask, coming1, coming2, coming3 = [], [], [], []
    for dy in (1, -1):
        here, there = min(EDGE[dy][0], BEHIND[dy][0]), min(EDGE[dy][1], BEHIND[dy][1])
        coming_mask.append(send(mask_view.at[lines(here, 2), line], mask_view.at[lines(there, 2), line], (dy, 0)))
    for dy in (1, -1):
        (here, there), run = EDGE[dy], pl.ds(*Y_RUN[dy])
        coming1.append(send(views[0].at[run, lines(here), line], views[0].at[run, lines(there), line], (dy, 0)))

    def half(dy):
        return (slice(planes, 2 * planes), slice(0, planes)) if dy == 1 else (slice(0, planes), slice(planes, 2 * planes))

    middle, ends = slice(1, SEG - 1), (slice(0, 1), slice(SEG - 1, SEG))

    def shifted(rows, by=LO):
        return slice(rows.start + by, rows.stop + by)

    first_rows(low + 1, high - 1)
    for y in (low, low + 1, high - 1, high):
        move_mask(y)
    for i, dy in enumerate((1, -1)):
        for p in range(planes):
            f = streamed(0, p, EDGE[dy][0], PART[dy])
            for n, k in enumerate(PART[dy]):
                part_e[i, n, p] = f[k]
        coming2.append(send(part_e.at[i, :, :, middle], part_h.at[i, :, :, middle], (dy, 0)))
    first_rows(low + 2, high - 2)
    for y in (low + 2, high - 2):
        move_mask(y)
    for i, dy in enumerate((1, -1)):
        here, there = BEHIND[dy]
        run = pl.ds(*Y_RUN[dy])
        for p in range(planes):
            f = collide(streamed(0, p, here), force)
            for n, k in enumerate(Y_SET[dy]):
                third_e[i, n, p] = f[k]
        coming3.append(send(third_e.at[i, :, :, middle], views[1].at[run, lines(there), shifted(middle)], (dy, 0)))

    def rest(y, carry):
        first_rows(y)
        return carry

    lax.fori_loop(low + 3, high - 2, rest, 0)

    arrive(coming_z)

    def every_row(p):
        return pl.ds(spot(low) + p, SEG, stride=planes)

    for p in range(planes):
        value = unpack(mzh, 0, p)
        strip_mask[every_row(p), :] = value
        mask[pl.ds(at(low, p, LO - 1), SEG, stride=planes * ROWS), :] = value
        mask[pl.ds(at(low, p, HI), SEG, stride=planes * ROWS), :] = value
    for t, tile in enumerate(tiles):
        for j, (p, k) in enumerate(tile):
            strip0[SLOT[k], every_row(p), :] = unpack(zh, t, j)
    for y in own_pairs:
        strip_relax(0, [strip0[SLOT[k], strip_rows(y), :] for k in range(19)], y)
    for y in range(low, high + 1):
        move_mask(y)

    for i, dy in enumerate((1, -1)):
        for p in range(planes):
            f = streamed(0, p, EDGE[dy][0], PART[dy])
            for n, k in enumerate(PART[dy]):
                part[i, n, p] = f[k]
        for rows in ends:
            coming2.append(send(part.at[i, :, :, rows], part_h.at[i, :, :, rows], (dy, 0)))
    for dy in (1, -1):
        flag_strip(pair_of(EDGE[dy][0]), PART[dy])
    for i, dy in enumerate((1, -1)):
        here, there = EDGE[dy]
        run = pl.ds(*Y_RUN[dy])
        f = strip_streamed(0, pair_of(here), PART[dy])
        for n, k in enumerate(PART[dy]):
            spart[i, n] = f[k]
        coming2.append(send(spart.at[i, :, half(dy)[0]], spart_h.at[i, :, half(dy)[0]], (dy, 0)))
        coming1.append(send(strip0.at[run, pl.ds(spot(here), planes)], strip0.at[run, pl.ds(spot(there), planes)], (dy, 0)))
        a, b = pair_of(here), pair_of(there)
        coming_mask.append(send(strip_mask.at[strip_rows(a)], strip_mask.at[strip_rows(b)], (dy, 0)))
    for i, dy in enumerate((1, -1)):
        here, there = BEHIND[dy]
        run = pl.ds(*Y_RUN[dy])
        advance(1, here)
        for rows in ends:
            rows = shifted(rows)
            coming3.append(send(views[1].at[run, lines(here), rows], views[1].at[run, lines(there), rows], (dy, 0)))
    for y in range(low + 1, high, 2):
        flag_strip(y)
        strip_advance(1, y)
    for i, dy in enumerate((1, -1)):
        here, there = BEHIND[dy]
        for n, k in enumerate(Y_SET[dy]):
            third[i, n] = strip1[SLOT[k], strip_rows(pair_of(here)), :]
        coming3.append(send(third.at[i, :, half(dy)[1]], third_h.at[i, :, half(dy)[1]], (dy, 0)))

    def over(first_row, last_row, block):
        def body(y, carry):
            block(y)
            return carry

        lax.fori_loop(first_row, last_row + 1, body, 0)

    over(low + 2, high - 2, functools.partial(advance, 1))
    over(low + 2, high - 2, functools.partial(advance, 2))
    for y in own_pairs[1:-1]:
        flag_strip(y)
        strip_advance(2, y)
    over(low + 3, high - 3, final)

    arrive(coming_mask)
    for dy in (1, -1):
        y = pair_of(EDGE[dy][1])
        value = strip_mask[strip_rows(y), :]
        mask[every_line(y, LO - 1), :] = value
        mask[every_line(y, HI), :] = value
        for there in (EDGE[dy][1], BEHIND[dy][1]):
            move_mask(there)
    for y in all_pairs:
        if y not in own_pairs[1:-1]:
            flag_strip(y)
    arrive(coming1)
    for dy in (1, -1):
        y = pair_of(EDGE[dy][1])
        for k in Y_SET[dy]:
            attach(cells0, k, y, strip0[SLOT[k], strip_rows(y), :])

    def finish(halves, i, dy, y):
        for p in range(planes):
            f = streamed(0, p, y, Y_SET[-dy])
            f.update({k: halves[i, n, p] for n, k in enumerate(PART[dy])})
            relax(1, f, p, y)

    for i, dy in enumerate((1, -1)):
        finish(part, i, dy, EDGE[dy][0])
        strip_advance(1, pair_of(EDGE[dy][0]))
    for dy in (1, -1):
        advance(2, BEHIND[dy][0])

    arrive(coming2)
    for i, dy in enumerate((1, -1)):
        y = EDGE[dy][1]
        finish(part_h, i, dy, y)
        y = pair_of(y)
        f = strip_streamed(0, y, Y_SET[-dy])
        f.update({k: spart_h[i, n] for n, k in enumerate(PART[dy])})
        strip_relax(1, f, y)
    for dy in (1, -1):
        advance(2, EDGE[dy][0])
        strip_advance(2, pair_of(EDGE[dy][0]))
    for y in (low + 1, low + 2, high - 2, high - 1):
        final(y)

    arrive(coming3)
    for i, dy in enumerate((1, -1)):
        y, behind = EDGE[dy][1], BEHIND[dy][1]
        pair = pair_of(y)
        for n, k in enumerate(Y_SET[dy]):
            strip1[SLOT[k], pl.ds(spot(behind), planes), :] = third_h[i, n, half(dy)[1], :]
            if velocities[k][2]:
                attach(cells1, k, pair, strip1[SLOT[k], strip_rows(pair), :])
        for p in range(planes):
            relax(2, streamed(1, p, y), p, y, Y_SET[dy])
        strip_advance(2, pair)
        final(low if dy == 1 else high)
    for copy in sent:
        copy.wait_send()


def hand_out(both_ref, den_hbm, vel_hbm, sem):
    den = pltpu.make_async_copy(both_ref.at[0], den_hbm, sem.at[0])
    vel = pltpu.make_async_copy(both_ref.at[pl.ds(1, 3)], vel_hbm, sem.at[1])
    vel.start()
    den.start()
    vel.wait()
    den.wait()


def solution(mesh):
    gy, gz = mesh.shape["gy"], mesh.shape["gz"]

    def tiles(x, across):
        lead = x.shape[:-2]
        x = x.reshape(*lead, across, SEG, W)
        return jnp.swapaxes(x, -3, -2).reshape(*lead, SEG * across, W)

    def lines(x, across):
        lead = x.shape[:-2]
        x = x.reshape(*lead, SEG, across, W)
        return jnp.swapaxes(x, -3, -2).reshape(*lead, across, SEG * W)

    def local(populations, solid_mask, body_force):
        planes, across, length = solid_mask.shape
        if length != SEG * W or across != SEG or 2 * planes != SEG:
            raise ValueError("unsupported block")
        messages = 48
        total = across + 2 * DEEP
        entries = (total * planes + 2 * SPARE) * ROWS
        strip = total * planes + 2 * SEG
        packs = -(-19 * planes // (W // STRIP))
        both = pl.pallas_call(
            functools.partial(kernel, gy, gz),
            out_shape=pltpu.VMEM((4, planes, SEG * across, W), jnp.float32),
            in_specs=[pl.BlockSpec(memory_space=pltpu.HBM)] * 3,
            out_specs=pl.BlockSpec(memory_space=pltpu.VMEM),
            scratch_shapes=[
                pltpu.VMEM((19, planes, SEG * across, W), jnp.float32),
                pltpu.VMEM((planes, SEG * across, W), jnp.int32),
                pltpu.SMEM((3,), jnp.float32),
                *[pltpu.VMEM((19, entries, W), jnp.float32)] * STEPS,
                *[pltpu.VMEM((19, strip, W), jnp.float32)] * (STEPS - 1),
                pltpu.VMEM((entries, W), jnp.int32),
                pltpu.VMEM((2, total, planes, SEG, W), jnp.int32),
                pltpu.VMEM((strip, W), jnp.int32),
                pltpu.VMEM((19, total, SEG, W), jnp.int32),
                *[pltpu.VMEM((2, packs, SEG, W), jnp.float32)] * 2,
                *[pltpu.VMEM((2, 1, SEG, W), jnp.int32)] * 2,
                *[pltpu.VMEM((2, 14, planes, SEG, W), jnp.float32)] * 3,
                pltpu.VMEM((2, 5, planes, SEG, W), jnp.float32),
                *[pltpu.VMEM((2, 14, SEG, W), jnp.float32)] * 2,
                *[pltpu.VMEM((2, 5, SEG, W), jnp.float32)] * 2,
                pltpu.SemaphoreType.DMA((2 + planes,)),
                pltpu.SemaphoreType.DMA((messages,)),
                pltpu.SemaphoreType.DMA((messages,)),
            ],
            compiler_params=pltpu.CompilerParams(collective_id=0, has_side_effects=True, vmem_limit_bytes=VMEM_LIMIT),
        )(*[pltpu.with_memory_space_constraint(x, pltpu.HBM) for x in (tiles(populations, across), tiles(solid_mask, across), body_force)])
        density, velocity = pl.pallas_call(
            hand_out,
            out_shape=(
                jax.ShapeDtypeStruct((planes, SEG * across, W), jnp.float32),
                jax.ShapeDtypeStruct((3, planes, SEG * across, W), jnp.float32),
            ),
            in_specs=[pl.BlockSpec(memory_space=pltpu.VMEM)],
            out_specs=(pl.BlockSpec(memory_space=pl.ANY), pl.BlockSpec(memory_space=pl.ANY)),
            scratch_shapes=[pltpu.SemaphoreType.DMA((2,))],
            compiler_params=pltpu.CompilerParams(vmem_limit_bytes=1 << 20),
        )(both)
        return lines(density, across), lines(velocity, across)

    return jax.shard_map(
        local,
        mesh=mesh,
        in_specs=(P(None, None, "gy", "gz"), P(None, "gy", "gz"), P()),
        out_specs=(P(None, "gy", "gz"), P(None, None, "gy", "gz")),
        check_vma=False,
    )
```

```python
import functools

import jax
import jax.numpy as jnp
from jax import lax
from jax.experimental import pallas as pl
from jax.experimental.pallas import tpu as pltpu
from jax.sharding import PartitionSpec as P

STEPS = 3
W = 128
SEG = 8
VMEM_LIMIT = 60 << 20
LO, HI, ROWS = 8, 16, 24
DEEP, STRIP, SPARE = 2, 3, 5

velocities = [
    (0, 0, 0),
    (1, 0, 0),
    (-1, 0, 0),
    (0, 1, 0),
    (0, -1, 0),
    (0, 0, 1),
    (0, 0, -1),
    (1, 1, 0),
    (-1, -1, 0),
    (1, -1, 0),
    (-1, 1, 0),
    (1, 0, 1),
    (-1, 0, -1),
    (1, 0, -1),
    (-1, 0, 1),
    (0, 1, 1),
    (0, -1, -1),
    (0, 1, -1),
    (0, -1, 1),
]
opposite = [0, 2, 1, 4, 3, 6, 5, 8, 7, 10, 9, 12, 11, 14, 13, 16, 15, 18, 17]
reference_mach = 0.05
ORDER = [5, 11, 14, 15, 3, 7, 10, 17, 6, 12, 13, 16, 4, 8, 9, 18, 0, 1, 2]
SLOT = [ORDER.index(k) for k in range(19)]
Y_RUN = {1: (3, 5), -1: (11, 5)}
Y_SET = {dy: [k for k in ORDER if velocities[k][1] == dy] for dy in (1, -1)}
PART = {dy: [k for k in ORDER if velocities[k][1] != -dy] for dy in (1, -1)}
SIDES = [(1, 0), (-1, 0), (0, 1), (0, -1)]
MESH = pl.DeviceIdType.MESH


def moments(f):
    s = [f[2 * a + 1] + f[2 * a + 2] for a in range(9)]
    d = [f[2 * a + 1] - f[2 * a + 2] for a in range(9)]
    axes = s[0] + s[1] + s[2]
    a = (s[3] + s[4], s[5] + s[6], s[7] + s[8])
    edges = a[0] + a[1] + a[2]
    rho = f[0] + axes + edges
    px, py, pz = (d[3] + d[4]) + (d[5] + d[6]), (d[3] - d[4]) + (d[7] + d[8]), (d[5] - d[6]) + (d[7] - d[8])
    jx, jy, jz = d[0] + px, d[1] + py, d[2] + pz
    return s, d, a, (axes, edges), (px, py, pz), rho, jx, jy, jz


def collide(f, force):
    s, d, (axy, axz, ayz), (axes, edges), p, rho, jx, jy, jz = moments(f)
    w = 0.3125 / rho
    vx, vy, vz = jx * w, jy * w, jz * w
    rx, ry, rz = jx * vx, jy * vy, jz * vz
    r = rx + ry + rz
    r3 = r * (0.325 / 0.9375)
    common = rho * (0.625 / 3.0 - 1.3 / 9.0) - r3
    fourth = rho * (0.325 / 9.0) + r3
    out = [None] * 19
    out[0] = (rho * (1.3 / 3.0 - 0.25) - r * 1.92) + (axes * 0.25 + edges * 0.2)
    g = [j * (0.4 / 3.0) + force[i][0] for i, j in enumerate((jx, jy, jz))]
    along = (axy + axz, axy + ayz, axz + ayz)
    for i, ri in enumerate((rx, ry, rz)):
        even = (common + ri * 0.96) + (along[i] * 0.025 - s[i] * 0.125)
        odd = (p[i] * 0.3 - g[i] * 0.25) + force[i][1]
        out[2 * i + 1] = even + odd
        out[2 * i + 2] = even - odd
    planes = (
        (3, axy, rz, vx * jy, g[0], g[1]),
        (5, axz, ry, vx * jz, g[0], g[2]),
        (7, ayz, rx, vy * jz, g[1], g[2]),
    )
    for n, total, across, shear, ga, gb in planes:
        a = (fourth - across * 0.52) - total * 0.075
        b = shear - (s[n] - s[n + 1]) * 0.0625
        e0, e1 = a + b, a - b
        o0, o1 = (ga + gb) - d[n] * 0.3, (ga - gb) - d[n + 1] * 0.3
        out[2 * n + 1], out[2 * n + 2] = e0 + o0, e0 - o0
        out[2 * n + 3], out[2 * n + 4] = e1 + o1, e1 - o1
    return out


def kernel(gy, gz, pop_hbm, mask_hbm, force_hbm, out_ref, raw, raw_mask, force_ref, cells0, cells1, cells2, strip0, strip1,
           mask, moved_mask, strip_mask, strip_flag, zs, zh, mzs, mzh, part_e, part, part_h, spart, spart_h,
           third, third_h,
           load_sem, send_sem, recv_sem):
    state, strips = (cells0, cells1, cells2), (strip0, strip1)
    planes, across = pop_hbm.shape[1], pop_hbm.shape[2] // SEG
    total = across + 2 * DEEP
    my, mz = lax.axis_index("gy"), lax.axis_index("gz")

    def peer(dy, dz):
        return {"gy": lax.rem(my + dy + gy, gy), "gz": lax.rem(mz + dz + gz, gz)}

    load_mask = pltpu.make_async_copy(mask_hbm, raw_mask, load_sem.at[0])
    load_force = pltpu.make_async_copy(force_hbm, force_ref, load_sem.at[1])
    load_pop = [pltpu.make_async_copy(pop_hbm.at[:, p], raw.at[:, p], load_sem.at[2 + p]) for p in range(planes)]
    load_mask.start()
    load_force.start()
    for copy in load_pop:
        copy.start()
    barrier = pltpu.get_barrier_semaphore()
    for dy, dz in SIDES:
        pl.semaphore_signal(barrier, inc=1, device_id=peer(dy, dz), device_id_type=MESH)

    lane = lax.broadcasted_iota(jnp.int32, (SEG, W), 1)
    plane_of = lax.rem(lax.broadcasted_iota(jnp.int32, (SEG, W), 0), planes)
    triple = (lane * 43) >> 7
    line = slice(LO, HI)
    count = [0]
    sent = []

    def send(source, target, side):
        copy = pltpu.make_async_remote_copy(
            src_ref=source,
            dst_ref=target,
            send_sem=send_sem.at[count[0]],
            recv_sem=recv_sem.at[count[0]],
            device_id=peer(*side),
            device_id_type=MESH,
        )
        count[0] += 1
        copy.start()
        sent.append(copy)
        return copy

    def arrive(copies):
        for copy in copies:
            copy.wait_recv()

    def view(ref, lead):
        return ref.reshape(*lead, total * planes + 2 * SPARE, ROWS, W)

    views = [view(ref, (19,)) for ref in state]
    mask_view = view(mask, ())

    def at(y, p, row=LO):
        return ((y * planes + p) + SPARE) * ROWS + row

    def lines(y, n=1):
        return pl.ds(y * planes + SPARE, n * planes)

    def spot(y):
        return SEG + y * planes

    low, high = DEEP, across + DEEP - 1
    EDGE = {1: (high, low - 1), -1: (low, high + 1)}
    BEHIND = {1: (high - 1, low - 2), -1: (low + 1, high + 2)}
    own_pairs = list(range(DEEP, DEEP + across, 2))
    all_pairs = list(range(0, total, 2))

    def pair_of(y):
        return y - y % 2

    def along_z(load, cz):
        v = load(0)
        if cz == 1:
            return pltpu.roll(jnp.where(lane == W - 1, load(-1), v), 1, 1)
        if cz == -1:
            return pltpu.roll(jnp.where(lane == 0, load(1), v), W - 1, 1)
        return v

    def move_mask(y):
        for p in range(planes):
            for i, cz in enumerate((1, -1)):
                moved_mask[i, y, p] = along_z(lambda o: mask[pl.ds(at(y, p, LO + o), SEG), :], cz)

    def streamed(step, p, y, ks=range(19)):
        f = {}
        for k in ks:
            cx, cy, cz = velocities[k]
            here = state[step][SLOT[opposite[k]], pl.ds(at(y, p), SEG), :]
            q = p - cx
            if k == 0 or not 0 <= q < planes:
                f[k] = here
                continue
            moved = along_z(lambda o: state[step][SLOT[k], pl.ds(at(y - cy, q, LO + o), SEG), :], cz)
            blocked = mask[pl.ds(at(y - cy, q), SEG), :] if cz == 0 else moved_mask[(1 - cz) // 2, y - cy, q]
            f[k] = jnp.where(blocked != 0, here, moved)
        return f

    def relax(step, f, p, y, ks=range(19)):
        out = collide(f, force)
        for k in ks:
            state[step][SLOT[k], pl.ds(at(y, p), SEG), :] = out[k]

    def advance(step, y):
        for p in range(planes):
            relax(step, streamed(step - 1, p, y), p, y)

    def final(y):
        for p in range(planes):
            rho, jx, jy, jz = moments(streamed(STEPS - 1, p, y))[-4:]
            fluid = (1 - mask[pl.ds(at(y, p), SEG), :]).astype(jnp.float32)
            scale = fluid * (1.0 / reference_mach) / rho
            rows = pl.ds(y - DEEP, SEG, stride=across)
            out_ref[0, p, rows, :] = rho * fluid
            out_ref[1, p, rows, :] = jx * scale
            out_ref[2, p, rows, :] = jy * scale
            out_ref[3, p, rows, :] = jz * scale

    def strip_rows(y):
        return pl.ds(spot(y), SEG)

    def every_line(y, row):
        return pl.ds(at(y, 0, row), SEG, stride=ROWS)

    def strip_move(ref_strip, ref_lines, y, c):
        cx, cy, cz = c
        v = ref_strip(strip_rows(y - cy))
        if cz == 1:
            v = pltpu.roll(jnp.where(lane == W - 1, ref_lines(every_line(y - cy, HI - 1)), v), 1, 1)
        elif cz == -1:
            v = pltpu.roll(jnp.where(lane == 0, ref_lines(every_line(y - cy, LO)), v), W - 1, 1)
        return pltpu.roll(v, cx % SEG, 0) if cx else v

    def flag_strip(y, ks=range(19)):
        for k in ks:
            cx = velocities[k][0]
            if k == 0:
                continue
            v = strip_move(lambda rows: strip_mask[rows, :], lambda rows: mask[rows, :], y, velocities[k])
            if cx:
                v = jnp.where(plane_of == (0 if cx == 1 else planes - 1), 1, v)
            strip_flag[k, y] = v

    def strip_streamed(step, y, ks=range(19)):
        f = {}
        for k in ks:
            slot = SLOT[k]
            here = strips[step][SLOT[opposite[k]], strip_rows(y), :]
            if k == 0:
                f[k] = here
                continue
            moved = strip_move(
                lambda rows: strips[step][slot, rows, :], lambda rows: state[step][slot, rows, :], y, velocities[k]
            )
            f[k] = jnp.where(strip_flag[k, y] != 0, here, moved)
        return f

    def attach(ref, k, y, value):
        cz = velocities[k][2]
        if cz:
            ref[SLOT[k], every_line(y, LO - 1 if cz == 1 else HI), :] = value

    def strip_relax(step, f, y):
        out = collide(f, force)
        for k in range(19):
            if step < STEPS - 1:
                strips[step][SLOT[k], strip_rows(y), :] = out[k]
            attach(state[step], k, y, out[k])

    def strip_advance(step, y):
        strip_relax(step, strip_streamed(step - 1, y), y)

    load_mask.wait()
    for p in range(planes):
        for y in range(across):
            mask[pl.ds(at(y + DEEP, p), SEG), :] = raw_mask[p, pl.ds(y, SEG, stride=across), :]
    load_force.wait()
    force = [(force_ref[i] * (1.0 / 12.0), force_ref[i] * 0.1875) for i in range(3)]

    def first(p, y):
        f = [raw[k, p, pl.ds(y - DEEP, SEG, stride=across), :] for k in range(19)]
        for k, value in enumerate(collide(f, force)):
            state[0][SLOT[k], pl.ds(at(y, p), SEG), :] = value

    def first_rows(*rows):
        for y in rows:
            for p in range(planes):
                first(p, y)

    for p in range(planes):
        load_pop[p].wait()
        first(p, low)
        first(p, high)

    groups = [(p, k) for p in range(planes) for k in range(19)]
    per_tile = W // STRIP

    def pack(out, tile, i, loads):
        end = pl.ds((SEG - 1) * across, across) if i == 0 else pl.ds(0, across)
        packed = jnp.zeros((SEG, W), out.dtype)
        for j, load in enumerate(loads):
            shift = (STRIP * j + (STRIP if i == 0 else 0)) % W
            v = load(end)
            packed = jnp.where(triple == j, pltpu.roll(v, shift, 1) if shift else v, packed)
        out[i, tile] = packed

    def unpack(into, tile, j):
        left, right = into[0, tile], into[1, tile]
        a, b = (W - STRIP - STRIP * j) % W, (W - STRIP * j) % W
        left = pltpu.roll(left, a, 1) if a else left
        right = pltpu.roll(right, b, 1) if b else right
        return jnp.where(lane < W // 2, right, left)

    tiles = [groups[n : n + per_tile] for n in range(0, len(groups), per_tile)]
    for i in range(2):
        pack(mzs, 0, i, [lambda end, p=p: raw_mask[p, end, :] for p in range(planes)])
        for t, tile in enumerate(tiles):
            pack(zs, t, i, [lambda end, p=p, k=k: raw[k, p, end, :] for p, k in tile])

    pl.semaphore_wait(barrier, len(SIDES))
    coming_z = []
    for i, dz in enumerate((1, -1)):
        coming_z.append(send(mzs.at[i], mzh.at[i], (0, dz)))
        coming_z.append(send(zs.at[i], zh.at[i], (0, dz)))
    coming_mask, coming1, coming2, coming3 = [], [], [], []
    for dy in (1, -1):
        here, there = min(EDGE[dy][0], BEHIND[dy][0]), min(EDGE[dy][1], BEHIND[dy][1])
        coming_mask.append(send(mask_view.at[lines(here, 2), line], mask_view.at[lines(there, 2), line], (dy, 0)))
    for dy in (1, -1):
        (here, there), run = EDGE[dy], pl.ds(*Y_RUN[dy])
        coming1.append(send(views[0].at[run, lines(here), line], views[0].at[run, lines(there), line], (dy, 0)))

    def half(dy):
        return (slice(planes, 2 * planes), slice(0, planes)) if dy == 1 else (slice(0, planes), slice(planes, 2 * planes))

    middle, ends = slice(1, SEG - 1), (slice(0, 1), slice(SEG - 1, SEG))

    first_rows(low + 1, high - 1)
    for y in (low, low + 1, high - 1, high):
        move_mask(y)
    for i, dy in enumerate((1, -1)):
        for p in range(planes):
            f = streamed(0, p, EDGE[dy][0], PART[dy])
            for n, k in enumerate(PART[dy]):
                part_e[i, n, p] = f[k]
        coming2.append(send(part_e.at[i, :, :, middle], part_h.at[i, :, :, middle], (dy, 0)))
    first_rows(low + 2, high - 2)
    def rest(y, carry):
        first_rows(y)
        return carry

    lax.fori_loop(low + 3, high - 2, rest, 0)

    arrive(coming_z)

    def every_row(p):
        return pl.ds(spot(low) + p, SEG, stride=planes)

    for p in range(planes):
        value = unpack(mzh, 0, p)
        strip_mask[every_row(p), :] = value
        mask[pl.ds(at(low, p, LO - 1), SEG, stride=planes * ROWS), :] = value
        mask[pl.ds(at(low, p, HI), SEG, stride=planes * ROWS), :] = value
    for t, tile in enumerate(tiles):
        for j, (p, k) in enumerate(tile):
            strip0[SLOT[k], every_row(p), :] = unpack(zh, t, j)
    for y in own_pairs:
        strip_relax(0, [strip0[SLOT[k], strip_rows(y), :] for k in range(19)], y)
    for y in range(low, high + 1):
        move_mask(y)

    def side_by_side(values):
        packed = jnp.zeros((SEG, W), jnp.float32)
        for j, v in enumerate(values):
            packed = jnp.where((triple >> 1) == j, pltpu.roll(v, (2 * STRIP * j + STRIP) % W, 1), packed)
        return packed

    def apart(packed, j):
        return pltpu.roll(packed, (W - STRIP - 2 * STRIP * j) % W, 1)

    for i, dy in enumerate((1, -1)):
        for p in range(planes):
            f = streamed(0, p, EDGE[dy][0], PART[dy])
            for n, k in enumerate(PART[dy]):
                part[i, n, p] = f[k]
        for rows in ends:
            coming2.append(send(part.at[i, :, :, rows], part_h.at[i, :, :, rows], (dy, 0)))
    for dy in (1, -1):
        flag_strip(pair_of(EDGE[dy][0]), PART[dy])
    for i, dy in enumerate((1, -1)):
        here, there = EDGE[dy]
        run = pl.ds(*Y_RUN[dy])
        y = pair_of(here)
        f = strip_streamed(0, y, PART[dy])
        values = [strip0[SLOT[k], strip_rows(y), :] for k in Y_SET[dy]] + [f[k] for k in PART[dy]]
        spart[i] = side_by_side(values)
        rows = half(dy)[0]
        coming1.append(send(spart.at[i, rows], spart_h.at[i, rows], (dy, 0)))
        a, b = pair_of(here), pair_of(there)
        coming_mask.append(send(strip_mask.at[strip_rows(a)], strip_mask.at[strip_rows(b)], (dy, 0)))
    for i, dy in enumerate((1, -1)):
        here, there = BEHIND[dy]
        run = pl.ds(*Y_RUN[dy])
        advance(1, here)
        coming3.append(send(views[1].at[run, lines(here), line], views[1].at[run, lines(there), line], (dy, 0)))
    for y in range(low + 1, high, 2):
        flag_strip(y)
        strip_advance(1, y)
    for i, dy in enumerate((1, -1)):
        here, there = BEHIND[dy]
        third[i] = side_by_side([strip1[SLOT[k], strip_rows(pair_of(here)), :] for k in Y_SET[dy]])
        rows = half(dy)[1]
        coming3.append(send(third.at[i, rows], third_h.at[i, rows], (dy, 0)))

    def over(first_row, last_row, block):
        def body(y, carry):
            block(y)
            return carry

        lax.fori_loop(first_row, last_row + 1, body, 0)

    over(low + 2, high - 2, functools.partial(advance, 1))
    over(low + 2, high - 2, functools.partial(advance, 2))
    for y in own_pairs[1:-1]:
        flag_strip(y)
        strip_advance(2, y)
    over(low + 3, high - 3, final)

    arrive(coming_mask)
    for dy in (1, -1):
        y = pair_of(EDGE[dy][1])
        value = strip_mask[strip_rows(y), :]
        mask[every_line(y, LO - 1), :] = value
        mask[every_line(y, HI), :] = value
        for there in (EDGE[dy][1], BEHIND[dy][1]):
            move_mask(there)
    for y in all_pairs:
        if y not in own_pairs[1:-1]:
            flag_strip(y)
    arrive(coming1)
    for i, dy in enumerate((1, -1)):
        y = pair_of(EDGE[dy][1])
        for n, k in enumerate(Y_SET[dy]):
            value = apart(spart_h[i], n)
            strip0[SLOT[k], strip_rows(y), :] = value
            attach(cells0, k, y, value)

    def finish(halves, i, dy, y):
        for p in range(planes):
            f = streamed(0, p, y, Y_SET[-dy])
            f.update({k: halves[i, n, p] for n, k in enumerate(PART[dy])})
            relax(1, f, p, y)

    for i, dy in enumerate((1, -1)):
        finish(part, i, dy, EDGE[dy][0])
        strip_advance(1, pair_of(EDGE[dy][0]))
    for dy in (1, -1):
        advance(2, BEHIND[dy][0])
    for y in (low + 1, high - 2):
        strip_advance(2, y)
    for y in (low + 2, high - 2):
        final(y)

    arrive(coming2)
    for i, dy in enumerate((1, -1)):
        y = EDGE[dy][1]
        finish(part_h, i, dy, y)
        y = pair_of(y)
        f = strip_streamed(0, y, Y_SET[-dy])
        f.update({k: apart(spart_h[i], len(Y_SET[dy]) + n) for n, k in enumerate(PART[dy])})
        strip_relax(1, f, y)
    for dy in (1, -1):
        advance(2, EDGE[dy][0])
        strip_advance(2, pair_of(EDGE[dy][0]))
    for y in (low + 1, high - 1):
        final(y)

    arrive(coming3)
    for i, dy in enumerate((1, -1)):
        y, behind = EDGE[dy][1], BEHIND[dy][1]
        pair = pair_of(y)
        for n, k in enumerate(Y_SET[dy]):
            strip1[SLOT[k], pl.ds(spot(behind), planes), :] = apart(third_h[i], n)[half(dy)[1], :]
            if velocities[k][2]:
                attach(cells1, k, pair, strip1[SLOT[k], strip_rows(pair), :])
        for p in range(planes):
            relax(2, streamed(1, p, y), p, y, Y_SET[dy])
        strip_advance(2, pair)
        final(low if dy == 1 else high)
    for copy in sent:
        copy.wait_send()


def hand_out(both_ref, den_hbm, vel_hbm, sem):
    den = pltpu.make_async_copy(both_ref.at[0], den_hbm, sem.at[0])
    vel = pltpu.make_async_copy(both_ref.at[pl.ds(1, 3)], vel_hbm, sem.at[1])
    vel.start()
    den.start()
    vel.wait()
    den.wait()


def solution(mesh):
    gy, gz = mesh.shape["gy"], mesh.shape["gz"]

    def tiles(x, across):
        lead = x.shape[:-2]
        x = x.reshape(*lead, across, SEG, W)
        return jnp.swapaxes(x, -3, -2).reshape(*lead, SEG * across, W)

    def lines(x, across):
        lead = x.shape[:-2]
        x = x.reshape(*lead, SEG, across, W)
        return jnp.swapaxes(x, -3, -2).reshape(*lead, across, SEG * W)

    def local(populations, solid_mask, body_force):
        planes, across, length = solid_mask.shape
        if length != SEG * W or across != SEG or 2 * planes != SEG:
            raise ValueError("unsupported block")
        messages = 48
        total = across + 2 * DEEP
        entries = (total * planes + 2 * SPARE) * ROWS
        strip = total * planes + 2 * SEG
        packs = -(-19 * planes // (W // STRIP))
        both = pl.pallas_call(
            functools.partial(kernel, gy, gz),
            out_shape=pltpu.VMEM((4, planes, SEG * across, W), jnp.float32),
            in_specs=[pl.BlockSpec(memory_space=pltpu.HBM)] * 3,
            out_specs=pl.BlockSpec(memory_space=pltpu.VMEM),
            scratch_shapes=[
                pltpu.VMEM((19, planes, SEG * across, W), jnp.float32),
                pltpu.VMEM((planes, SEG * across, W), jnp.int32),
                pltpu.SMEM((3,), jnp.float32),
                *[pltpu.VMEM((19, entries, W), jnp.float32)] * STEPS,
                *[pltpu.VMEM((19, strip, W), jnp.float32)] * (STEPS - 1),
                pltpu.VMEM((entries, W), jnp.int32),
                pltpu.VMEM((2, total, planes, SEG, W), jnp.int32),
                pltpu.VMEM((strip, W), jnp.int32),
                pltpu.VMEM((19, total, SEG, W), jnp.int32),
                *[pltpu.VMEM((2, packs, SEG, W), jnp.float32)] * 2,
                *[pltpu.VMEM((2, 1, SEG, W), jnp.int32)] * 2,
                *[pltpu.VMEM((2, 14, planes, SEG, W), jnp.float32)] * 3,
                *[pltpu.VMEM((2, SEG, W), jnp.float32)] * 4,
                pltpu.SemaphoreType.DMA((2 + planes,)),
                pltpu.SemaphoreType.DMA((messages,)),
                pltpu.SemaphoreType.DMA((messages,)),
            ],
            compiler_params=pltpu.CompilerParams(collective_id=0, has_side_effects=True, vmem_limit_bytes=VMEM_LIMIT),
        )(*[pltpu.with_memory_space_constraint(x, pltpu.HBM) for x in (tiles(populations, across), tiles(solid_mask, across), body_force)])
        density, velocity = pl.pallas_call(
            hand_out,
            out_shape=(
                jax.ShapeDtypeStruct((planes, SEG * across, W), jnp.float32),
                jax.ShapeDtypeStruct((3, planes, SEG * across, W), jnp.float32),
            ),
            in_specs=[pl.BlockSpec(memory_space=pltpu.VMEM)],
            out_specs=(pl.BlockSpec(memory_space=pl.ANY), pl.BlockSpec(memory_space=pl.ANY)),
            scratch_shapes=[pltpu.SemaphoreType.DMA((2,))],
            compiler_params=pltpu.CompilerParams(vmem_limit_bytes=1 << 20),
        )(both)
        return lines(density, across), lines(velocity, across)

    return jax.shard_map(
        local,
        mesh=mesh,
        in_specs=(P(None, None, "gy", "gz"), P(None, "gy", "gz"), P()),
        out_specs=(P(None, "gy", "gz"), P(None, None, "gy", "gz")),
        check_vma=False,
    )
```

```python
import functools

import jax
import jax.numpy as jnp
from jax import lax
from jax.experimental import pallas as pl
from jax.experimental.pallas import tpu as pltpu
from jax.sharding import PartitionSpec as P

STEPS = 3
W = 128
SEG = 8
VMEM_LIMIT = 60 << 20
LO, HI, ROWS = 8, 16, 24
DEEP, STRIP, SPARE = 2, 3, 5

velocities = [
    (0, 0, 0),
    (1, 0, 0),
    (-1, 0, 0),
    (0, 1, 0),
    (0, -1, 0),
    (0, 0, 1),
    (0, 0, -1),
    (1, 1, 0),
    (-1, -1, 0),
    (1, -1, 0),
    (-1, 1, 0),
    (1, 0, 1),
    (-1, 0, -1),
    (1, 0, -1),
    (-1, 0, 1),
    (0, 1, 1),
    (0, -1, -1),
    (0, 1, -1),
    (0, -1, 1),
]
opposite = [0, 2, 1, 4, 3, 6, 5, 8, 7, 10, 9, 12, 11, 14, 13, 16, 15, 18, 17]
reference_mach = 0.05
ORDER = [5, 11, 14, 15, 3, 7, 10, 17, 6, 12, 13, 16, 4, 8, 9, 18, 0, 1, 2]
SLOT = [ORDER.index(k) for k in range(19)]
Y_RUN = {1: (3, 5), -1: (11, 5)}
Y_SET = {dy: [k for k in ORDER if velocities[k][1] == dy] for dy in (1, -1)}
PART = {dy: [k for k in ORDER if velocities[k][1] != -dy] for dy in (1, -1)}
SIDES = [(1, 0), (-1, 0), (0, 1), (0, -1)]
MESH = pl.DeviceIdType.MESH
SIDE = {1: 0, -1: 1}


def moments(f):
    s = [f[2 * a + 1] + f[2 * a + 2] for a in range(9)]
    d = [f[2 * a + 1] - f[2 * a + 2] for a in range(9)]
    axes = s[0] + s[1] + s[2]
    a = (s[3] + s[4], s[5] + s[6], s[7] + s[8])
    edges = a[0] + a[1] + a[2]
    rho = f[0] + axes + edges
    px, py, pz = (d[3] + d[4]) + (d[5] + d[6]), (d[3] - d[4]) + (d[7] + d[8]), (d[5] - d[6]) + (d[7] - d[8])
    jx, jy, jz = d[0] + px, d[1] + py, d[2] + pz
    return s, d, a, (axes, edges), (px, py, pz), rho, jx, jy, jz


def collide(f, force):
    s, d, (axy, axz, ayz), (axes, edges), p, rho, jx, jy, jz = moments(f)
    w = 0.3125 / rho
    vx, vy, vz = jx * w, jy * w, jz * w
    rx, ry, rz = jx * vx, jy * vy, jz * vz
    r = rx + ry + rz
    r3 = r * (0.325 / 0.9375)
    common = rho * (0.625 / 3.0 - 1.3 / 9.0) - r3
    fourth = rho * (0.325 / 9.0) + r3
    out = [None] * 19
    out[0] = (rho * (1.3 / 3.0 - 0.25) - r * 1.92) + (axes * 0.25 + edges * 0.2)
    g = [j * (0.4 / 3.0) + force[i][0] for i, j in enumerate((jx, jy, jz))]
    along = (axy + axz, axy + ayz, axz + ayz)
    for i, ri in enumerate((rx, ry, rz)):
        even = (common + ri * 0.96) + (along[i] * 0.025 - s[i] * 0.125)
        odd = (p[i] * 0.3 - g[i] * 0.25) + force[i][1]
        out[2 * i + 1] = even + odd
        out[2 * i + 2] = even - odd
    planes = (
        (3, axy, rz, vx * jy, g[0], g[1]),
        (5, axz, ry, vx * jz, g[0], g[2]),
        (7, ayz, rx, vy * jz, g[1], g[2]),
    )
    for n, total, across, shear, ga, gb in planes:
        a = (fourth - across * 0.52) - total * 0.075
        b = shear - (s[n] - s[n + 1]) * 0.0625
        e0, e1 = a + b, a - b
        o0, o1 = (ga + gb) - d[n] * 0.3, (ga - gb) - d[n + 1] * 0.3
        out[2 * n + 1], out[2 * n + 2] = e0 + o0, e0 - o0
        out[2 * n + 3], out[2 * n + 4] = e1 + o1, e1 - o1
    return out


def kernel(gy, gz, pop_hbm, mask_hbm, force_hbm, out_ref, raw, raw_mask, force_ref, cells0, cells1, cells2, strip0, strip1,
           mask, moved_mask, strip_mask, strip_flag, zs, zh, mzs, mzh, part_e, part, part_h, spart, spart_h,
           third, third_h,
           load_sem, send_sem, recv_sem):
    state, strips = (cells0, cells1, cells2), (strip0, strip1)
    planes, across = pop_hbm.shape[1], pop_hbm.shape[2] // SEG
    total = across + 2 * DEEP
    my, mz = lax.axis_index("gy"), lax.axis_index("gz")

    def peer(dy, dz):
        return {"gy": lax.rem(my + dy + gy, gy), "gz": lax.rem(mz + dz + gz, gz)}

    load_mask = pltpu.make_async_copy(mask_hbm, raw_mask, load_sem.at[0])
    load_force = pltpu.make_async_copy(force_hbm, force_ref, load_sem.at[1])
    load_pop = [pltpu.make_async_copy(pop_hbm.at[:, p], raw.at[:, p], load_sem.at[2 + p]) for p in range(planes)]
    load_mask.start()
    load_force.start()
    for copy in load_pop:
        copy.start()
    barrier = pltpu.get_barrier_semaphore()
    for dy, dz in SIDES:
        pl.semaphore_signal(barrier, inc=1, device_id=peer(dy, dz), device_id_type=MESH)

    lane = lax.broadcasted_iota(jnp.int32, (SEG, W), 1)
    plane_of = lax.rem(lax.broadcasted_iota(jnp.int32, (SEG, W), 0), planes)
    triple = (lane * 43) >> 7
    line = slice(LO, HI)
    count = [0]
    sent = []

    def send(source, target, side):
        copy = pltpu.make_async_remote_copy(
            src_ref=source,
            dst_ref=target,
            send_sem=send_sem.at[count[0]],
            recv_sem=recv_sem.at[count[0]],
            device_id=peer(*side),
            device_id_type=MESH,
        )
        count[0] += 1
        copy.start()
        sent.append(copy)
        return copy

    def arrive(copies):
        for copy in copies:
            copy.wait_recv()

    def view(ref, lead):
        return ref.reshape(*lead, total * planes + 2 * SPARE, ROWS, W)

    views = [view(ref, (19,)) for ref in state]
    mask_view = view(mask, ())

    def at(y, p, row=LO):
        return ((y * planes + p) + SPARE) * ROWS + row

    def lines(y, n=1):
        return pl.ds(y * planes + SPARE, n * planes)

    def spot(y):
        return SEG + y * planes

    low, high = DEEP, across + DEEP - 1
    EDGE = {1: (high, low - 1), -1: (low, high + 1)}
    BEHIND = {1: (high - 1, low - 2), -1: (low + 1, high + 2)}
    own_pairs = list(range(DEEP, DEEP + across, 2))
    all_pairs = list(range(0, total, 2))

    def pair_of(y):
        return y - y % 2

    def along_z(load, cz):
        v = load(0)
        if cz == 1:
            return pltpu.roll(jnp.where(lane == W - 1, load(-1), v), 1, 1)
        if cz == -1:
            return pltpu.roll(jnp.where(lane == 0, load(1), v), W - 1, 1)
        return v

    def move_mask(y):
        for p in range(planes):
            for i, cz in enumerate((1, -1)):
                moved_mask[i, y, p] = along_z(lambda o: mask[pl.ds(at(y, p, LO + o), SEG), :], cz)

    def streamed(step, p, y, ks=range(19)):
        f = {}
        for k in ks:
            cx, cy, cz = velocities[k]
            here = state[step][SLOT[opposite[k]], pl.ds(at(y, p), SEG), :]
            q = p - cx
            if k == 0 or not 0 <= q < planes:
                f[k] = here
                continue
            moved = along_z(lambda o: state[step][SLOT[k], pl.ds(at(y - cy, q, LO + o), SEG), :], cz)
            blocked = mask[pl.ds(at(y - cy, q), SEG), :] if cz == 0 else moved_mask[(1 - cz) // 2, y - cy, q]
            f[k] = jnp.where(blocked != 0, here, moved)
        return f

    def relax(step, f, p, y, ks=range(19)):
        out = collide(f, force)
        for k in ks:
            state[step][SLOT[k], pl.ds(at(y, p), SEG), :] = out[k]

    def advance(step, y):
        for p in range(planes):
            relax(step, streamed(step - 1, p, y), p, y)

    def final(y):
        for p in range(planes):
            rho, jx, jy, jz = moments(streamed(STEPS - 1, p, y))[-4:]
            fluid = (1 - mask[pl.ds(at(y, p), SEG), :]).astype(jnp.float32)
            scale = fluid * (1.0 / reference_mach) / rho
            rows = pl.ds(y - DEEP, SEG, stride=across)
            out_ref[0, p, rows, :] = rho * fluid
            out_ref[1, p, rows, :] = jx * scale
            out_ref[2, p, rows, :] = jy * scale
            out_ref[3, p, rows, :] = jz * scale

    def strip_rows(y):
        return pl.ds(spot(y), SEG)

    def every_line(y, row):
        return pl.ds(at(y, 0, row), SEG, stride=ROWS)

    def strip_move(ref_strip, ref_lines, y, c):
        cx, cy, cz = c
        v = ref_strip(strip_rows(y - cy))
        if cz == 1:
            v = pltpu.roll(jnp.where(lane == W - 1, ref_lines(every_line(y - cy, HI - 1)), v), 1, 1)
        elif cz == -1:
            v = pltpu.roll(jnp.where(lane == 0, ref_lines(every_line(y - cy, LO)), v), W - 1, 1)
        return pltpu.roll(v, cx % SEG, 0) if cx else v

    def flag_strip(y, ks=range(19)):
        for k in ks:
            cx = velocities[k][0]
            if k == 0:
                continue
            v = strip_move(lambda rows: strip_mask[rows, :], lambda rows: mask[rows, :], y, velocities[k])
            if cx:
                v = jnp.where(plane_of == (0 if cx == 1 else planes - 1), 1, v)
            strip_flag[k, y] = v

    def strip_streamed(step, y, ks=range(19)):
        f = {}
        for k in ks:
            slot = SLOT[k]
            here = strips[step][SLOT[opposite[k]], strip_rows(y), :]
            if k == 0:
                f[k] = here
                continue
            moved = strip_move(
                lambda rows: strips[step][slot, rows, :], lambda rows: state[step][slot, rows, :], y, velocities[k]
            )
            f[k] = jnp.where(strip_flag[k, y] != 0, here, moved)
        return f

    def attach(ref, k, y, value):
        cz = velocities[k][2]
        if cz:
            ref[SLOT[k], every_line(y, LO - 1 if cz == 1 else HI), :] = value

    def strip_relax(step, f, y):
        out = collide(f, force)
        for k in range(19):
            if step < STEPS - 1:
                strips[step][SLOT[k], strip_rows(y), :] = out[k]
            attach(state[step], k, y, out[k])

    def strip_advance(step, y):
        strip_relax(step, strip_streamed(step - 1, y), y)

    load_mask.wait()
    for p in range(planes):
        for y in range(across):
            mask[pl.ds(at(y + DEEP, p), SEG), :] = raw_mask[p, pl.ds(y, SEG, stride=across), :]
    load_force.wait()
    force = [(force_ref[i] * (1.0 / 12.0), force_ref[i] * 0.1875) for i in range(3)]

    def first(p, y):
        f = [raw[k, p, pl.ds(y - DEEP, SEG, stride=across), :] for k in range(19)]
        for k, value in enumerate(collide(f, force)):
            state[0][SLOT[k], pl.ds(at(y, p), SEG), :] = value

    def first_rows(*rows):
        for y in rows:
            for p in range(planes):
                first(p, y)

    for p in range(planes):
        load_pop[p].wait()
        first(p, low)
        first(p, high)

    groups = [(p, k) for p in range(planes) for k in range(19)]
    per_tile = W // STRIP

    def pack(out, tile, i, loads):
        end = pl.ds((SEG - 1) * across, across) if i == 0 else pl.ds(0, across)
        packed = jnp.zeros((SEG, W), out.dtype)
        for j, load in enumerate(loads):
            shift = (STRIP * j + (STRIP if i == 0 else 0)) % W
            v = load(end)
            packed = jnp.where(triple == j, pltpu.roll(v, shift, 1) if shift else v, packed)
        out[i, tile] = packed

    def unpack(into, tile, j):
        left, right = into[0, tile], into[1, tile]
        a, b = (W - STRIP - STRIP * j) % W, (W - STRIP * j) % W
        left = pltpu.roll(left, a, 1) if a else left
        right = pltpu.roll(right, b, 1) if b else right
        return jnp.where(lane < W // 2, right, left)

    tiles = [groups[n : n + per_tile] for n in range(0, len(groups), per_tile)]
    for i in range(2):
        pack(mzs, 0, i, [lambda end, p=p: raw_mask[p, end, :] for p in range(planes)])
        for t, tile in enumerate(tiles):
            pack(zs, t, i, [lambda end, p=p, k=k: raw[k, p, end, :] for p, k in tile])

    pl.semaphore_wait(barrier, len(SIDES))
    coming_z = []
    for i, dz in enumerate((1, -1)):
        coming_z.append(send(mzs.at[i], mzh.at[i], (0, dz)))
        coming_z.append(send(zs.at[i], zh.at[i], (0, dz)))
    coming_mask, coming1, coming2, coming3 = ({1: [], -1: []} for _ in range(4))
    for dy in (1, -1):
        here, there = min(EDGE[dy][0], BEHIND[dy][0]), min(EDGE[dy][1], BEHIND[dy][1])
        coming_mask[dy].append(send(mask_view.at[lines(here, 2), line], mask_view.at[lines(there, 2), line], (dy, 0)))
    for dy in (1, -1):
        (here, there), run = EDGE[dy], pl.ds(*Y_RUN[dy])
        coming1[dy].append(send(views[0].at[run, lines(here), line], views[0].at[run, lines(there), line], (dy, 0)))

    def half(dy):
        return (slice(planes, 2 * planes), slice(0, planes)) if dy == 1 else (slice(0, planes), slice(planes, 2 * planes))

    middle, ends = slice(1, SEG - 1), (slice(0, 1), slice(SEG - 1, SEG))

    first_rows(low + 1, high - 1)
    for y in (low, low + 1, high - 1, high):
        move_mask(y)
    for i, dy in enumerate((1, -1)):
        for p in range(planes):
            f = streamed(0, p, EDGE[dy][0], PART[dy])
            for n, k in enumerate(PART[dy]):
                part_e[i, n, p] = f[k]
        coming2[dy].append(send(part_e.at[i, :, :, middle], part_h.at[i, :, :, middle], (dy, 0)))
    first_rows(low + 2, high - 2)
    def rest(y, carry):
        first_rows(y)
        return carry

    lax.fori_loop(low + 3, high - 2, rest, 0)

    arrive(coming_z)

    def every_row(p):
        return pl.ds(spot(low) + p, SEG, stride=planes)

    for p in range(planes):
        value = unpack(mzh, 0, p)
        strip_mask[every_row(p), :] = value
        mask[pl.ds(at(low, p, LO - 1), SEG, stride=planes * ROWS), :] = value
        mask[pl.ds(at(low, p, HI), SEG, stride=planes * ROWS), :] = value
    for t, tile in enumerate(tiles):
        for j, (p, k) in enumerate(tile):
            strip0[SLOT[k], every_row(p), :] = unpack(zh, t, j)
    for y in own_pairs:
        strip_relax(0, [strip0[SLOT[k], strip_rows(y), :] for k in range(19)], y)
    for y in range(low, high + 1):
        move_mask(y)

    def side_by_side(values):
        packed = jnp.zeros((SEG, W), jnp.float32)
        for j, v in enumerate(values):
            packed = jnp.where((triple >> 1) == j, pltpu.roll(v, (2 * STRIP * j + STRIP) % W, 1), packed)
        return packed

    def apart(packed, j):
        return pltpu.roll(packed, (W - STRIP - 2 * STRIP * j) % W, 1)

    for i, dy in enumerate((1, -1)):
        for p in range(planes):
            f = streamed(0, p, EDGE[dy][0], PART[dy])
            for n, k in enumerate(PART[dy]):
                part[i, n, p] = f[k]
        for rows in ends:
            coming2[dy].append(send(part.at[i, :, :, rows], part_h.at[i, :, :, rows], (dy, 0)))
    for dy in (1, -1):
        flag_strip(pair_of(EDGE[dy][0]), PART[dy])
    for i, dy in enumerate((1, -1)):
        here, there = EDGE[dy]
        run = pl.ds(*Y_RUN[dy])
        y = pair_of(here)
        f = strip_streamed(0, y, PART[dy])
        values = [strip0[SLOT[k], strip_rows(y), :] for k in Y_SET[dy]] + [f[k] for k in PART[dy]]
        spart[i] = side_by_side(values)
        rows = half(dy)[0]
        coming1[dy].append(send(spart.at[i, rows], spart_h.at[i, rows], (dy, 0)))
        a, b = pair_of(here), pair_of(there)
        coming_mask[dy].append(send(strip_mask.at[strip_rows(a)], strip_mask.at[strip_rows(b)], (dy, 0)))
    for i, dy in enumerate((1, -1)):
        here, there = BEHIND[dy]
        run = pl.ds(*Y_RUN[dy])
        advance(1, here)
        coming3[dy].append(send(views[1].at[run, lines(here), line], views[1].at[run, lines(there), line], (dy, 0)))
    for y in range(low + 1, high, 2):
        flag_strip(y)
        strip_advance(1, y)
    for i, dy in enumerate((1, -1)):
        here, there = BEHIND[dy]
        third[i] = side_by_side([strip1[SLOT[k], strip_rows(pair_of(here)), :] for k in Y_SET[dy]])
        rows = half(dy)[1]
        coming3[dy].append(send(third.at[i, rows], third_h.at[i, rows], (dy, 0)))

    def over(first_row, last_row, block):
        def body(y, carry):
            block(y)
            return carry

        lax.fori_loop(first_row, last_row + 1, body, 0)

    over(low + 2, high - 2, functools.partial(advance, 1))
    over(low + 2, high - 2, functools.partial(advance, 2))
    for y in own_pairs[1:-1]:
        flag_strip(y)
        strip_advance(2, y)
    over(low + 3, high - 3, final)

    def finish(halves, dy, y):
        for p in range(planes):
            f = streamed(0, p, y, Y_SET[-dy])
            f.update({k: halves[SIDE[dy], n, p] for n, k in enumerate(PART[dy])})
            relax(1, f, p, y)

    def close(away):
        i = SIDE[away]
        edge, halo = EDGE[-away][0], EDGE[away][1]
        behind, beyond = BEHIND[-away][0], BEHIND[away][1]
        third_row = behind - (edge - behind)
        pair, outer = pair_of(edge), pair_of(halo)
        arrive(coming_mask[away])
        value = strip_mask[strip_rows(outer), :]
        mask[every_line(outer, LO - 1), :] = value
        mask[every_line(outer, HI), :] = value
        move_mask(halo)
        move_mask(beyond)
        flag_strip(pair)
        flag_strip(outer)
        arrive(coming1[away])
        for n, k in enumerate(Y_SET[away]):
            value = apart(spart_h[i], n)
            strip0[SLOT[k], strip_rows(outer), :] = value
            attach(cells0, k, outer, value)
        finish(part, -away, edge)
        strip_advance(1, pair)
        advance(2, behind)
        strip_advance(2, min(behind, third_row))
        final(third_row)
        arrive(coming2[away])
        finish(part_h, away, halo)
        f = strip_streamed(0, outer, Y_SET[-away])
        f.update({k: apart(spart_h[i], len(Y_SET[away]) + n) for n, k in enumerate(PART[away])})
        strip_relax(1, f, outer)
        advance(2, edge)
        strip_advance(2, pair)
        final(behind)
        arrive(coming3[away])
        for n, k in enumerate(Y_SET[away]):
            strip1[SLOT[k], pl.ds(spot(beyond), planes), :] = apart(third_h[i], n)[half(away)[1], :]
            if velocities[k][2]:
                attach(cells1, k, outer, strip1[SLOT[k], strip_rows(outer), :])
        for p in range(planes):
            relax(2, streamed(1, p, halo), p, halo, Y_SET[away])
        strip_advance(2, outer)
        final(edge)

    odd = lax.rem(my, 2) == 1

    @pl.when(odd)
    def _():
        close(1)
        close(-1)

    @pl.when(jnp.logical_not(odd))
    def _():
        close(-1)
        close(1)

    for copy in sent:
        copy.wait_send()


def hand_out(both_ref, den_hbm, vel_hbm, sem):
    den = pltpu.make_async_copy(both_ref.at[0], den_hbm, sem.at[0])
    vel = pltpu.make_async_copy(both_ref.at[pl.ds(1, 3)], vel_hbm, sem.at[1])
    vel.start()
    den.start()
    vel.wait()
    den.wait()


def solution(mesh):
    gy, gz = mesh.shape["gy"], mesh.shape["gz"]

    def tiles(x, across):
        lead = x.shape[:-2]
        x = x.reshape(*lead, across, SEG, W)
        return jnp.swapaxes(x, -3, -2).reshape(*lead, SEG * across, W)

    def lines(x, across):
        lead = x.shape[:-2]
        x = x.reshape(*lead, SEG, across, W)
        return jnp.swapaxes(x, -3, -2).reshape(*lead, across, SEG * W)

    def local(populations, solid_mask, body_force):
        planes, across, length = solid_mask.shape
        if length != SEG * W or across != SEG or 2 * planes != SEG:
            raise ValueError("unsupported block")
        messages = 48
        total = across + 2 * DEEP
        entries = (total * planes + 2 * SPARE) * ROWS
        strip = total * planes + 2 * SEG
        packs = -(-19 * planes // (W // STRIP))
        both = pl.pallas_call(
            functools.partial(kernel, gy, gz),
            out_shape=pltpu.VMEM((4, planes, SEG * across, W), jnp.float32),
            in_specs=[pl.BlockSpec(memory_space=pltpu.HBM)] * 3,
            out_specs=pl.BlockSpec(memory_space=pltpu.VMEM),
            scratch_shapes=[
                pltpu.VMEM((19, planes, SEG * across, W), jnp.float32),
                pltpu.VMEM((planes, SEG * across, W), jnp.int32),
                pltpu.SMEM((3,), jnp.float32),
                *[pltpu.VMEM((19, entries, W), jnp.float32)] * STEPS,
                *[pltpu.VMEM((19, strip, W), jnp.float32)] * (STEPS - 1),
                pltpu.VMEM((entries, W), jnp.int32),
                pltpu.VMEM((2, total, planes, SEG, W), jnp.int32),
                pltpu.VMEM((strip, W), jnp.int32),
                pltpu.VMEM((19, total, SEG, W), jnp.int32),
                *[pltpu.VMEM((2, packs, SEG, W), jnp.float32)] * 2,
                *[pltpu.VMEM((2, 1, SEG, W), jnp.int32)] * 2,
                *[pltpu.VMEM((2, 14, planes, SEG, W), jnp.float32)] * 3,
                *[pltpu.VMEM((2, SEG, W), jnp.float32)] * 4,
                pltpu.SemaphoreType.DMA((2 + planes,)),
                pltpu.SemaphoreType.DMA((messages,)),
                pltpu.SemaphoreType.DMA((messages,)),
            ],
            compiler_params=pltpu.CompilerParams(collective_id=0, has_side_effects=True, vmem_limit_bytes=VMEM_LIMIT),
        )(*[pltpu.with_memory_space_constraint(x, pltpu.HBM) for x in (tiles(populations, across), tiles(solid_mask, across), body_force)])
        density, velocity = pl.pallas_call(
            hand_out,
            out_shape=(
                jax.ShapeDtypeStruct((planes, SEG * across, W), jnp.float32),
                jax.ShapeDtypeStruct((3, planes, SEG * across, W), jnp.float32),
            ),
            in_specs=[pl.BlockSpec(memory_space=pltpu.VMEM)],
            out_specs=(pl.BlockSpec(memory_space=pl.ANY), pl.BlockSpec(memory_space=pl.ANY)),
            scratch_shapes=[pltpu.SemaphoreType.DMA((2,))],
            compiler_params=pltpu.CompilerParams(vmem_limit_bytes=1 << 20),
        )(both)
        return lines(density, across), lines(velocity, across)

    return jax.shard_map(
        local,
        mesh=mesh,
        in_specs=(P(None, None, "gy", "gz"), P(None, "gy", "gz"), P()),
        out_specs=(P(None, "gy", "gz"), P(None, None, "gy", "gz")),
        check_vma=False,
    )
```

```python
import functools

import jax
import jax.numpy as jnp
from jax import lax
from jax.experimental import pallas as pl
from jax.experimental.pallas import tpu as pltpu
from jax.sharding import PartitionSpec as P

STEPS = 3
W = 128
SEG = 8
VMEM_LIMIT = 60 << 20
LO, HI, ROWS = 8, 16, 24
DEEP, STRIP, SPARE = 2, 3, 5

velocities = [
    (0, 0, 0),
    (1, 0, 0),
    (-1, 0, 0),
    (0, 1, 0),
    (0, -1, 0),
    (0, 0, 1),
    (0, 0, -1),
    (1, 1, 0),
    (-1, -1, 0),
    (1, -1, 0),
    (-1, 1, 0),
    (1, 0, 1),
    (-1, 0, -1),
    (1, 0, -1),
    (-1, 0, 1),
    (0, 1, 1),
    (0, -1, -1),
    (0, 1, -1),
    (0, -1, 1),
]
opposite = [0, 2, 1, 4, 3, 6, 5, 8, 7, 10, 9, 12, 11, 14, 13, 16, 15, 18, 17]
reference_mach = 0.05
ORDER = [5, 11, 14, 15, 3, 17, 7, 10, 6, 12, 13, 16, 4, 18, 9, 8, 0, 1, 2]
SLOT = [ORDER.index(k) for k in range(19)]
Y_RUN = {1: (3, 5), -1: (11, 5)}
Y_SET = {dy: [k for k in ORDER if velocities[k][1] == dy] for dy in (1, -1)}
PART = {dy: [k for k in ORDER if velocities[k][1] != -dy] for dy in (1, -1)}
SIDES = [(1, 0), (-1, 0), (0, 1), (0, -1)]
MESH = pl.DeviceIdType.MESH
SIDE = {1: 0, -1: 1}


def moments(f):
    s = [f[2 * a + 1] + f[2 * a + 2] for a in range(9)]
    d = [f[2 * a + 1] - f[2 * a + 2] for a in range(9)]
    axes = s[0] + s[1] + s[2]
    a = (s[3] + s[4], s[5] + s[6], s[7] + s[8])
    edges = a[0] + a[1] + a[2]
    rho = f[0] + axes + edges
    px, py, pz = (d[3] + d[4]) + (d[5] + d[6]), (d[3] - d[4]) + (d[7] + d[8]), (d[5] - d[6]) + (d[7] - d[8])
    jx, jy, jz = d[0] + px, d[1] + py, d[2] + pz
    return s, d, a, (axes, edges), (px, py, pz), rho, jx, jy, jz


def collide(f, force):
    s, d, (axy, axz, ayz), (axes, edges), p, rho, jx, jy, jz = moments(f)
    w = 0.3125 / rho
    vx, vy, vz = jx * w, jy * w, jz * w
    rx, ry, rz = jx * vx, jy * vy, jz * vz
    r = rx + ry + rz
    r3 = r * (0.325 / 0.9375)
    common = rho * (0.625 / 3.0 - 1.3 / 9.0) - r3
    fourth = rho * (0.325 / 9.0) + r3
    out = [None] * 19
    out[0] = (rho * (1.3 / 3.0 - 0.25) - r * 1.92) + (axes * 0.25 + edges * 0.2)
    g = [j * (0.4 / 3.0) + force[i][0] for i, j in enumerate((jx, jy, jz))]
    along = (axy + axz, axy + ayz, axz + ayz)
    for i, ri in enumerate((rx, ry, rz)):
        even = (common + ri * 0.96) + (along[i] * 0.025 - s[i] * 0.125)
        odd = (p[i] * 0.3 - g[i] * 0.25) + force[i][1]
        out[2 * i + 1] = even + odd
        out[2 * i + 2] = even - odd
    planes = (
        (3, axy, rz, vx * jy, g[0], g[1]),
        (5, axz, ry, vx * jz, g[0], g[2]),
        (7, ayz, rx, vy * jz, g[1], g[2]),
    )
    for n, total, across, shear, ga, gb in planes:
        a = (fourth - across * 0.52) - total * 0.075
        b = shear - (s[n] - s[n + 1]) * 0.0625
        e0, e1 = a + b, a - b
        o0, o1 = (ga + gb) - d[n] * 0.3, (ga - gb) - d[n + 1] * 0.3
        out[2 * n + 1], out[2 * n + 2] = e0 + o0, e0 - o0
        out[2 * n + 3], out[2 * n + 4] = e1 + o1, e1 - o1
    return out


def kernel(gy, gz, pop_hbm, mask_hbm, force_hbm, out_ref, raw, raw_mask, force_ref, cells0, cells1, cells2, strip0, strip1,
           mask, moved_mask, strip_mask, strip_flag, zs, zh, mzs, mzh, part_e, part, part_h, spart, spart_h,
           third, third_h,
           load_sem, send_sem, recv_sem):
    state, strips = (cells0, cells1, cells2), (strip0, strip1)
    planes, across = pop_hbm.shape[1], pop_hbm.shape[2] // SEG
    total = across + 2 * DEEP
    my, mz = lax.axis_index("gy"), lax.axis_index("gz")

    def peer(dy, dz):
        return {"gy": lax.rem(my + dy + gy, gy), "gz": lax.rem(mz + dz + gz, gz)}

    load_mask = pltpu.make_async_copy(mask_hbm, raw_mask, load_sem.at[0])
    load_force = pltpu.make_async_copy(force_hbm, force_ref, load_sem.at[1])
    load_pop = [pltpu.make_async_copy(pop_hbm.at[:, p], raw.at[:, p], load_sem.at[2 + p]) for p in range(planes)]
    load_mask.start()
    load_force.start()
    for copy in load_pop:
        copy.start()
    barrier = pltpu.get_barrier_semaphore()
    for dy, dz in SIDES:
        pl.semaphore_signal(barrier, inc=1, device_id=peer(dy, dz), device_id_type=MESH)

    lane = lax.broadcasted_iota(jnp.int32, (SEG, W), 1)
    plane_of = lax.rem(lax.broadcasted_iota(jnp.int32, (SEG, W), 0), planes)
    triple = (lane * 43) >> 7
    line = slice(LO, HI)
    count = [0]
    sent = []

    def send(source, target, side):
        copy = pltpu.make_async_remote_copy(
            src_ref=source,
            dst_ref=target,
            send_sem=send_sem.at[count[0]],
            recv_sem=recv_sem.at[count[0]],
            device_id=peer(*side),
            device_id_type=MESH,
        )
        count[0] += 1
        copy.start()
        sent.append(copy)
        return copy

    def arrive(copies):
        for copy in copies:
            copy.wait_recv()

    def view(ref, lead):
        return ref.reshape(*lead, total * planes + 2 * SPARE, ROWS, W)

    views = [view(ref, (19,)) for ref in state]
    mask_view = view(mask, ())

    def at(y, p, row=LO):
        return ((y * planes + p) + SPARE) * ROWS + row

    def lines(y, n=1):
        return pl.ds(y * planes + SPARE, n * planes)

    def spot(y):
        return SEG + y * planes

    low, high = DEEP, across + DEEP - 1
    EDGE = {1: (high, low - 1), -1: (low, high + 1)}
    BEHIND = {1: (high - 1, low - 2), -1: (low + 1, high + 2)}
    own_pairs = list(range(DEEP, DEEP + across, 2))
    all_pairs = list(range(0, total, 2))

    def pair_of(y):
        return y - y % 2

    def along_z(load, cz):
        v = load(0)
        if cz == 1:
            return pltpu.roll(jnp.where(lane == W - 1, load(-1), v), 1, 1)
        if cz == -1:
            return pltpu.roll(jnp.where(lane == 0, load(1), v), W - 1, 1)
        return v

    def move_mask(y):
        for p in range(planes):
            for i, cz in enumerate((1, -1)):
                moved_mask[i, y, p] = along_z(lambda o: mask[pl.ds(at(y, p, LO + o), SEG), :], cz)

    def streamed(step, p, y, ks=range(19)):
        f = {}
        for k in ks:
            cx, cy, cz = velocities[k]
            here = state[step][SLOT[opposite[k]], pl.ds(at(y, p), SEG), :]
            q = p - cx
            if k == 0 or not 0 <= q < planes:
                f[k] = here
                continue
            moved = along_z(lambda o: state[step][SLOT[k], pl.ds(at(y - cy, q, LO + o), SEG), :], cz)
            blocked = mask[pl.ds(at(y - cy, q), SEG), :] if cz == 0 else moved_mask[(1 - cz) // 2, y - cy, q]
            f[k] = jnp.where(blocked != 0, here, moved)
        return f

    def relax(step, f, p, y, ks=range(19)):
        out = collide(f, force)
        for k in ks:
            state[step][SLOT[k], pl.ds(at(y, p), SEG), :] = out[k]

    def advance(step, y):
        for p in range(planes):
            relax(step, streamed(step - 1, p, y), p, y)

    def final(y):
        for p in range(planes):
            rho, jx, jy, jz = moments(streamed(STEPS - 1, p, y))[-4:]
            fluid = (1 - mask[pl.ds(at(y, p), SEG), :]).astype(jnp.float32)
            scale = fluid * (1.0 / reference_mach) / rho
            rows = pl.ds(y - DEEP, SEG, stride=across)
            out_ref[0, p, rows, :] = rho * fluid
            out_ref[1, p, rows, :] = jx * scale
            out_ref[2, p, rows, :] = jy * scale
            out_ref[3, p, rows, :] = jz * scale

    def strip_rows(y):
        return pl.ds(spot(y), SEG)

    def every_line(y, row):
        return pl.ds(at(y, 0, row), SEG, stride=ROWS)

    def strip_move(ref_strip, ref_lines, y, c):
        cx, cy, cz = c
        v = ref_strip(strip_rows(y - cy))
        if cz == 1:
            v = pltpu.roll(jnp.where(lane == W - 1, ref_lines(every_line(y - cy, HI - 1)), v), 1, 1)
        elif cz == -1:
            v = pltpu.roll(jnp.where(lane == 0, ref_lines(every_line(y - cy, LO)), v), W - 1, 1)
        return pltpu.roll(v, cx % SEG, 0) if cx else v

    def flag_strip(y, ks=range(19)):
        for k in ks:
            cx = velocities[k][0]
            if k == 0:
                continue
            v = strip_move(lambda rows: strip_mask[rows, :], lambda rows: mask[rows, :], y, velocities[k])
            if cx:
                v = jnp.where(plane_of == (0 if cx == 1 else planes - 1), 1, v)
            strip_flag[k, y] = v

    def strip_streamed(step, y, ks=range(19)):
        f = {}
        for k in ks:
            slot = SLOT[k]
            here = strips[step][SLOT[opposite[k]], strip_rows(y), :]
            if k == 0:
                f[k] = here
                continue
            moved = strip_move(
                lambda rows: strips[step][slot, rows, :], lambda rows: state[step][slot, rows, :], y, velocities[k]
            )
            f[k] = jnp.where(strip_flag[k, y] != 0, here, moved)
        return f

    def attach(ref, k, y, value):
        cz = velocities[k][2]
        if cz:
            ref[SLOT[k], every_line(y, LO - 1 if cz == 1 else HI), :] = value

    def strip_relax(step, f, y):
        out = collide(f, force)
        for k in range(19):
            if step < STEPS - 1:
                strips[step][SLOT[k], strip_rows(y), :] = out[k]
            attach(state[step], k, y, out[k])

    def strip_advance(step, y):
        strip_relax(step, strip_streamed(step - 1, y), y)

    load_mask.wait()
    for p in range(planes):
        for y in range(across):
            mask[pl.ds(at(y + DEEP, p), SEG), :] = raw_mask[p, pl.ds(y, SEG, stride=across), :]
    load_force.wait()
    force = [(force_ref[i] * (1.0 / 12.0), force_ref[i] * 0.1875) for i in range(3)]

    def first(p, y):
        f = [raw[k, p, pl.ds(y - DEEP, SEG, stride=across), :] for k in range(19)]
        for k, value in enumerate(collide(f, force)):
            state[0][SLOT[k], pl.ds(at(y, p), SEG), :] = value

    def first_rows(*rows):
        for y in rows:
            for p in range(planes):
                first(p, y)

    for p in range(planes):
        load_pop[p].wait()
        first(p, low)
        first(p, high)

    groups = [(p, k) for p in range(planes) for k in range(19)]
    per_tile = W // STRIP

    def pack(out, tile, i, loads):
        end = pl.ds((SEG - 1) * across, across) if i == 0 else pl.ds(0, across)
        packed = jnp.zeros((SEG, W), out.dtype)
        for j, load in enumerate(loads):
            shift = (STRIP * j + (STRIP if i == 0 else 0)) % W
            v = load(end)
            packed = jnp.where(triple == j, pltpu.roll(v, shift, 1) if shift else v, packed)
        out[i, tile] = packed

    def unpack(into, tile, j):
        left, right = into[0, tile], into[1, tile]
        a, b = (W - STRIP - STRIP * j) % W, (W - STRIP * j) % W
        left = pltpu.roll(left, a, 1) if a else left
        right = pltpu.roll(right, b, 1) if b else right
        return jnp.where(lane < W // 2, right, left)

    tiles = [groups[n : n + per_tile] for n in range(0, len(groups), per_tile)]
    for i in range(2):
        pack(mzs, 0, i, [lambda end, p=p: raw_mask[p, end, :] for p in range(planes)])
        for t, tile in enumerate(tiles):
            pack(zs, t, i, [lambda end, p=p, k=k: raw[k, p, end, :] for p, k in tile])

    pl.semaphore_wait(barrier, len(SIDES))
    coming_z = []
    for i, dz in enumerate((1, -1)):
        coming_z.append(send(mzs.at[i], mzh.at[i], (0, dz)))
        coming_z.append(send(zs.at[i], zh.at[i], (0, dz)))
    coming_mask, coming1, coming2, coming3 = ({1: [], -1: []} for _ in range(4))
    for dy in (1, -1):
        here, there = min(EDGE[dy][0], BEHIND[dy][0]), min(EDGE[dy][1], BEHIND[dy][1])
        coming_mask[dy].append(send(mask_view.at[lines(here, 2), line], mask_view.at[lines(there, 2), line], (dy, 0)))
    for dy in (1, -1):
        (here, there), run = EDGE[dy], pl.ds(*Y_RUN[dy])
        coming1[dy].append(send(views[0].at[run, lines(here), line], views[0].at[run, lines(there), line], (dy, 0)))

    def half(dy):
        return (slice(planes, 2 * planes), slice(0, planes)) if dy == 1 else (slice(0, planes), slice(planes, 2 * planes))

    middle, ends = slice(1, SEG - 1), (slice(0, 1), slice(SEG - 1, SEG))

    first_rows(low + 1, high - 1)
    for y in (low, low + 1, high - 1, high):
        move_mask(y)
    for i, dy in enumerate((1, -1)):
        for p in range(planes):
            f = streamed(0, p, EDGE[dy][0], PART[dy])
            for n, k in enumerate(PART[dy]):
                part_e[i, n, p] = f[k]
        coming2[dy].append(send(part_e.at[i, :, :, middle], part_h.at[i, :, :, middle], (dy, 0)))
    first_rows(low + 2, high - 2)
    def rest(y, carry):
        first_rows(y)
        return carry

    lax.fori_loop(low + 3, high - 2, rest, 0)

    arrive(coming_z)

    def every_row(p):
        return pl.ds(spot(low) + p, SEG, stride=planes)

    for p in range(planes):
        value = unpack(mzh, 0, p)
        strip_mask[every_row(p), :] = value
        mask[pl.ds(at(low, p, LO - 1), SEG, stride=planes * ROWS), :] = value
        mask[pl.ds(at(low, p, HI), SEG, stride=planes * ROWS), :] = value
    for t, tile in enumerate(tiles):
        for j, (p, k) in enumerate(tile):
            strip0[SLOT[k], every_row(p), :] = unpack(zh, t, j)
    for y in own_pairs:
        strip_relax(0, [strip0[SLOT[k], strip_rows(y), :] for k in range(19)], y)
    for y in range(low, high + 1):
        move_mask(y)

    def side_by_side(values):
        packed = jnp.zeros((SEG, W), jnp.float32)
        for j, v in enumerate(values):
            packed = jnp.where((triple >> 1) == j, pltpu.roll(v, (2 * STRIP * j + STRIP) % W, 1), packed)
        return packed

    def apart(packed, j):
        return pltpu.roll(packed, (W - STRIP - 2 * STRIP * j) % W, 1)

    for i, dy in enumerate((1, -1)):
        for p in range(planes):
            f = streamed(0, p, EDGE[dy][0], PART[dy])
            for n, k in enumerate(PART[dy]):
                part[i, n, p] = f[k]
        for rows in ends:
            coming2[dy].append(send(part.at[i, :, :, rows], part_h.at[i, :, :, rows], (dy, 0)))
    for dy in (1, -1):
        flag_strip(pair_of(EDGE[dy][0]), PART[dy])
    for i, dy in enumerate((1, -1)):
        here, there = EDGE[dy]
        run = pl.ds(*Y_RUN[dy])
        y = pair_of(here)
        f = strip_streamed(0, y, PART[dy])
        values = [strip0[SLOT[k], strip_rows(y), :] for k in Y_SET[dy]] + [f[k] for k in PART[dy]]
        spart[i] = side_by_side(values)
        rows = half(dy)[0]
        coming1[dy].append(send(spart.at[i, rows], spart_h.at[i, rows], (dy, 0)))
        a, b = pair_of(here), pair_of(there)
        coming_mask[dy].append(send(strip_mask.at[strip_rows(a)], strip_mask.at[strip_rows(b)], (dy, 0)))
    for i, dy in enumerate((1, -1)):
        here, there = BEHIND[dy]
        run = pl.ds(*Y_RUN[dy])
        advance(1, here)
        for n, count_k, p, count_p in ((0, 3, 0, planes), (3, 1, 0, planes - 1), (4, 1, 1, planes - 1)):
            slots = pl.ds(Y_RUN[dy][0] + n, count_k)
            source, target = (pl.ds(row * planes + SPARE + p, count_p) for row in (here, there))
            coming3[dy].append(send(views[1].at[slots, source, line], views[1].at[slots, target, line], (dy, 0)))
    for y in range(low + 1, high, 2):
        flag_strip(y)
        strip_advance(1, y)
    for i, dy in enumerate((1, -1)):
        here, there = BEHIND[dy]
        third[i] = side_by_side([strip1[SLOT[k], strip_rows(pair_of(here)), :] for k in Y_SET[dy]])
        rows = half(dy)[1]
        coming3[dy].append(send(third.at[i, rows], third_h.at[i, rows], (dy, 0)))

    def over(first_row, last_row, block):
        def body(y, carry):
            block(y)
            return carry

        lax.fori_loop(first_row, last_row + 1, body, 0)

    over(low + 2, high - 2, functools.partial(advance, 1))
    over(low + 2, high - 2, functools.partial(advance, 2))
    for y in own_pairs[1:-1]:
        flag_strip(y)
        strip_advance(2, y)
    over(low + 3, high - 3, final)

    def finish(halves, dy, y):
        for p in range(planes):
            f = streamed(0, p, y, Y_SET[-dy])
            f.update({k: halves[SIDE[dy], n, p] for n, k in enumerate(PART[dy])})
            relax(1, f, p, y)

    def close(away):
        i = SIDE[away]
        edge, halo = EDGE[-away][0], EDGE[away][1]
        behind, beyond = BEHIND[-away][0], BEHIND[away][1]
        third_row = behind - (edge - behind)
        pair, outer = pair_of(edge), pair_of(halo)
        arrive(coming_mask[away])
        value = strip_mask[strip_rows(outer), :]
        mask[every_line(outer, LO - 1), :] = value
        mask[every_line(outer, HI), :] = value
        move_mask(halo)
        move_mask(beyond)
        flag_strip(pair)
        flag_strip(outer)
        arrive(coming1[away])
        for n, k in enumerate(Y_SET[away]):
            value = apart(spart_h[i], n)
            strip0[SLOT[k], strip_rows(outer), :] = value
            attach(cells0, k, outer, value)
        finish(part, -away, edge)
        strip_advance(1, pair)
        advance(2, behind)
        strip_advance(2, min(behind, third_row))
        final(third_row)
        arrive(coming2[away])
        finish(part_h, away, halo)
        f = strip_streamed(0, outer, Y_SET[-away])
        f.update({k: apart(spart_h[i], len(Y_SET[away]) + n) for n, k in enumerate(PART[away])})
        strip_relax(1, f, outer)
        advance(2, edge)
        strip_advance(2, pair)
        final(behind)
        arrive(coming3[away])
        for n, k in enumerate(Y_SET[away]):
            strip1[SLOT[k], pl.ds(spot(beyond), planes), :] = apart(third_h[i], n)[half(away)[1], :]
            if velocities[k][2]:
                attach(cells1, k, outer, strip1[SLOT[k], strip_rows(outer), :])
        for p in range(planes):
            relax(2, streamed(1, p, halo), p, halo, Y_SET[away])
        strip_advance(2, outer)
        final(edge)

    odd = lax.rem(my, 2) == 1

    @pl.when(odd)
    def _():
        close(1)
        close(-1)

    @pl.when(jnp.logical_not(odd))
    def _():
        close(-1)
        close(1)

    for copy in sent:
        copy.wait_send()


def hand_out(both_ref, den_hbm, vel_hbm, sem):
    copies = [pltpu.make_async_copy(both_ref.at[0], den_hbm, sem.at[0])]
    copies += [pltpu.make_async_copy(both_ref.at[1 + i], vel_hbm.at[i], sem.at[1 + i]) for i in range(3)]
    for copy in copies:
        copy.start()
    for copy in copies:
        copy.wait()


def solution(mesh):
    gy, gz = mesh.shape["gy"], mesh.shape["gz"]

    def tiles(x, across):
        lead = x.shape[:-2]
        x = x.reshape(*lead, across, SEG, W)
        return jnp.swapaxes(x, -3, -2).reshape(*lead, SEG * across, W)

    def lines(x, across):
        lead = x.shape[:-2]
        x = x.reshape(*lead, SEG, across, W)
        return jnp.swapaxes(x, -3, -2).reshape(*lead, across, SEG * W)

    def local(populations, solid_mask, body_force):
        planes, across, length = solid_mask.shape
        if length != SEG * W or across != SEG or 2 * planes != SEG:
            raise ValueError("unsupported block")
        messages = 48
        total = across + 2 * DEEP
        entries = (total * planes + 2 * SPARE) * ROWS
        strip = total * planes + 2 * SEG
        packs = -(-19 * planes // (W // STRIP))
        both = pl.pallas_call(
            functools.partial(kernel, gy, gz),
            out_shape=pltpu.VMEM((4, planes, SEG * across, W), jnp.float32),
            in_specs=[pl.BlockSpec(memory_space=pltpu.HBM)] * 3,
            out_specs=pl.BlockSpec(memory_space=pltpu.VMEM),
            scratch_shapes=[
                pltpu.VMEM((19, planes, SEG * across, W), jnp.float32),
                pltpu.VMEM((planes, SEG * across, W), jnp.int32),
                pltpu.SMEM((3,), jnp.float32),
                *[pltpu.VMEM((19, entries, W), jnp.float32)] * STEPS,
                *[pltpu.VMEM((19, strip, W), jnp.float32)] * (STEPS - 1),
                pltpu.VMEM((entries, W), jnp.int32),
                pltpu.VMEM((2, total, planes, SEG, W), jnp.int32),
                pltpu.VMEM((strip, W), jnp.int32),
                pltpu.VMEM((19, total, SEG, W), jnp.int32),
                *[pltpu.VMEM((2, packs, SEG, W), jnp.float32)] * 2,
                *[pltpu.VMEM((2, 1, SEG, W), jnp.int32)] * 2,
                *[pltpu.VMEM((2, 14, planes, SEG, W), jnp.float32)] * 3,
                *[pltpu.VMEM((2, SEG, W), jnp.float32)] * 4,
                pltpu.SemaphoreType.DMA((2 + planes,)),
                pltpu.SemaphoreType.DMA((messages,)),
                pltpu.SemaphoreType.DMA((messages,)),
            ],
            compiler_params=pltpu.CompilerParams(collective_id=0, has_side_effects=True, vmem_limit_bytes=VMEM_LIMIT),
        )(*[pltpu.with_memory_space_constraint(x, pltpu.HBM) for x in (tiles(populations, across), tiles(solid_mask, across), body_force)])
        density, velocity = pl.pallas_call(
            hand_out,
            out_shape=(
                jax.ShapeDtypeStruct((planes, SEG * across, W), jnp.float32),
                jax.ShapeDtypeStruct((3, planes, SEG * across, W), jnp.float32),
            ),
            in_specs=[pl.BlockSpec(memory_space=pltpu.VMEM)],
            out_specs=(pl.BlockSpec(memory_space=pl.ANY), pl.BlockSpec(memory_space=pl.ANY)),
            scratch_shapes=[pltpu.SemaphoreType.DMA((4,))],
            compiler_params=pltpu.CompilerParams(vmem_limit_bytes=1 << 20),
        )(both)
        return lines(density, across), lines(velocity, across)

    return jax.shard_map(
        local,
        mesh=mesh,
        in_specs=(P(None, None, "gy", "gz"), P(None, "gy", "gz"), P()),
        out_specs=(P(None, "gy", "gz"), P(None, None, "gy", "gz")),
        check_vma=False,
    )
```
